32 devices in a mesh: dp: 4 (over z), expert: 8 (over y, x, core).
Axes of the slice: x: 2, y: 2, z: 4, core: 2. Of those that a mesh axis runs over, the one named last changes fastest.
Arguments:
- block_in: float32 [25216, 768], P(('dp', 'expert')), may hold values from -6 to 6
- out_grad: float32 [25216, 768], P(('dp', 'expert')), may hold values from -6 to 6
- expert_ids: int32 [25216, 2], P(('dp', 'expert')), may hold values from 0 to 15, as said below
- slot_ids: int32 [25216, 2], P(('dp', 'expert')), may hold values from -1 to 110, as said below
- qkv_weight: bfloat16 [768, 2304], P('dp'), may hold values from -0.21875 to 0.21875
- q_bias: bfloat16 [768], P('dp'), may hold values from -3 to 3
- v_bias: bfloat16 [768], P('dp'), may hold values from -3 to 3
- out_weight: bfloat16 [768, 768], P('dp'), may hold values from -0.875 to 0.875
- out_bias: bfloat16 [768], P('dp'), may hold values from -2 to 2
- norm1_gain: bfloat16 [768], P('dp'), may hold values from 0.5 to 1.5
- norm1_bias: bfloat16 [768], P('dp'), may hold values from -2 to 2
- norm2_gain: bfloat16 [768], P('dp'), may hold values from 0.5 to 1.5
- norm2_bias: bfloat16 [768], P('dp'), may hold values from -2 to 2
- router_weight: bfloat16 [768, 16], P('dp'), may hold values from -0.4375 to 0.4375
- up_weight: bfloat16 [16, 768, 3072], P('expert'), may hold values from -0.21875 to 0.21875
- up_bias: bfloat16 [16, 3072], P('expert'), may hold values from -3 to 3
- down_weight: bfloat16 [16, 3072, 768], P('expert'), may hold values from -2.5 to 2.5
- down_bias: bfloat16 [16, 768], P('expert'), may hold values from -10 to 10
Outputs:
- block_out: float32 [25216, 768], P(('dp', 'expert'))
- input_grad: float32 [25216, 768], P(('dp', 'expert'))
- qkv_weight_grad: float32 [768, 2304], P(('dp', 'expert'))
- q_bias_grad: float32 [768], P(('dp', 'expert'))
- v_bias_grad: float32 [768], P(('dp', 'expert'))
- out_weight_grad: float32 [768, 768], P(('dp', 'expert'))
- out_bias_grad: float32 [768], P(('dp', 'expert'))
- norm1_gain_grad: float32 [768], P(('dp', 'expert'))
- norm1_bias_grad: float32 [768], P(('dp', 'expert'))
- norm2_gain_grad: float32 [768], P(('dp', 'expert'))
- norm2_bias_grad: float32 [768], P(('dp', 'expert'))
- router_weight_grad: float32 [768, 16], P(('dp', 'expert'))
- up_weight_grad: float32 [16, 768, 3072], P('expert', 'dp')
- up_bias_grad: float32 [16, 3072], P('expert', 'dp')
- down_weight_grad: float32 [16, 3072, 768], P('expert', 'dp')
- down_bias_grad: float32 [16, 768], P('expert', 'dp')
The draws below stay inside these ranges and needn't reach their ends.
Inputs may be any that keep to these rules, and one draw needn't show every extreme that they name: `expert_ids`: the two experts of a token differ. `slot_ids`: within each block of 788 rows (the rows of one device), a choice's slot is its rank among the choices of that block naming the same expert, in a priority order where all first choices come before all second choices (the order among tokens is drawn); ranks of 111 or more are dropped and marked -1. Slots of one block and expert are distinct, and some expert fills all 111 slots in every block.
All inputs are finite; a program needn't handle non-finite values.
Results may differ from the reference program's by a relative error of at most 0.023.
Values may be sent and summed in bfloat16 or wider, within the bound.
A program may use at most 256 MiB of HBM per device.

```python
import jax
import jax.numpy as jnp
from jax import lax

D = 768
HEADS = 12
HEAD = 64
FF = 3072
SEQ = 197
TOP = 2
EXPERTS = 16
TOK_DEV = 788
TOKENS = 25216
CAP = 111
DEVICES = 32


def shuffle_block(subkey):
    return jax.random.permutation(subkey, TOK_DEV)


def block_slots(chosen, order_key):
    ordering = jnp.argsort(order_key, stable=True)
    sorted_experts = chosen[ordering]
    labels = jnp.arange(EXPERTS, dtype=jnp.int32)
    matches = (sorted_experts[:, None] == labels[None, :]).astype(jnp.int32)
    before = jnp.cumsum(matches, axis=0) - matches
    counted = jnp.sum(before * matches, axis=1)
    ranked = jnp.zeros_like(counted).at[ordering].set(counted)
    return jnp.where(ranked < CAP, ranked, -1).astype(jnp.int32)


def routing(key):
    base = jax.random.fold_in(key, 101)
    subkeys = jax.random.split(base, 7)
    hot_expert = jax.random.randint(subkeys[0], (), 0, EXPERTS)
    relabel = jax.random.permutation(subkeys[1], EXPERTS)
    draw_one = jax.random.randint(subkeys[2], (DEVICES, TOK_DEV), 0, EXPERTS)
    draw_two = jax.random.randint(subkeys[3], (DEVICES, TOK_DEV), 0, EXPERTS)
    first_choice = relabel[jnp.minimum(draw_one, draw_two)]
    forced_rank = jax.vmap(shuffle_block)(jax.random.split(subkeys[4], DEVICES))
    first_choice = jnp.where(forced_rank < CAP + CAP // 2, hot_expert, first_choice)
    offset = jax.random.randint(subkeys[5], (DEVICES, TOK_DEV), 1, EXPERTS)
    second_choice = (first_choice + offset) % EXPERTS
    priority = jax.vmap(shuffle_block)(jax.random.split(subkeys[6], DEVICES))
    chosen = jnp.stack([first_choice, second_choice], axis=-1).astype(jnp.int32)
    order_key = priority[:, :, None] + TOK_DEV * jnp.arange(2, dtype=jnp.int32)[None, None, :]
    slots = jax.vmap(block_slots)(chosen.reshape(DEVICES, TOK_DEV * 2), order_key.reshape(DEVICES, TOK_DEV * 2).astype(jnp.int32))
    return (chosen.reshape(TOKENS, 2), slots.reshape(TOKENS, 2))


def draw_expert_ids(key, part):
    return routing(key)[0]


def draw_slot_ids(key, part):
    return routing(key)[1]


def spiked(result, rng, source, target, blocks, factor):
    def block_of(position):
        return (jnp.arange(result.shape[position]) // (result.shape[position] // blocks)).reshape((-1,) + (1,) * (result.ndim - 1 - position))

    one_side = jax.random.permutation(rng, blocks)[block_of(target)]
    second = (block_of(target) + blocks // 2) % blocks
    return jnp.where((block_of(source) == one_side) | (block_of(source) == second), factor * result, result)


def block_levels(own_key, shape, cuts, smallest, top_value):
    def one(dim, shards_of):
        heights = jax.random.uniform(jax.random.fold_in(jax.random.fold_in(own_key, 6), dim), (shards_of,), jnp.float32, smallest / len(cuts), top_value / len(cuts))
        return jnp.repeat(jnp.exp(heights), shape[dim] // shards_of).reshape((-1,) + (1,) * (len(shape) - dim - 1))

    loudness = one(*cuts[0])
    for cut in cuts[1:]:
        loudness = loudness * one(*cut)
    return loudness


def normal_values(rng, extent, scale, bound, pieces=(), kind=jnp.bfloat16):
    result = jax.random.normal(rng, extent, jnp.float32) * scale
    if len(pieces) > 0:
        result = block_levels(rng, extent, pieces, -0.22, 0.18) * result
    return jnp.clip(result, min=-bound, max=bound).astype(kind)


def bell_draw_with(key, extent, spread, limit, shards, heavy, held_as=jnp.bfloat16):
    entries = spread * jax.random.normal(key, extent, jnp.float32)
    if shards:
        entries = entries * block_levels(key, extent, shards, -0.22, 0.18)
    return jnp.clip(spiked(entries, jax.random.fold_in(key, 3), *heavy), -limit, limit).astype(held_as)


def setup_inputs(seed: int = 0) -> dict:
    arg_keys = jax.random.split(jax.random.key(seed), 19)
    return {
        "block_in": normal_values(arg_keys[0], (TOKENS, D), 1.0, 6.0, ((0, 32),), jnp.float32),
        "out_grad": bell_draw_with(arg_keys[1], (TOKENS, D), 1.0, 6.0, ((0, 32),), (0, 1, 32, 2.75), jnp.float32),
        "expert_ids": draw_expert_ids(jax.random.fold_in(arg_keys[18], 71), 0),
        "slot_ids": draw_slot_ids(jax.random.fold_in(arg_keys[18], 71), 0),
        "qkv_weight": normal_values(arg_keys[4], (D, 3 * D), D ** -0.5, 0.21875, ((0, 4),)),
        "q_bias": normal_values(arg_keys[5], (D,), 0.5, 3.0, ((0, 4),)),
        "v_bias": normal_values(arg_keys[6], (D,), 0.5, 3.0, ((0, 4),)),
        "out_weight": normal_values(arg_keys[7], (D, D), (D // 14) ** -0.5, 0.875, ((0, 4),)),
        "out_bias": normal_values(arg_keys[8], (D,), 0.3, 2.0, ((0, 4),)),
        "norm1_gain": jnp.clip(1.0 + 0.1 * jax.random.normal(arg_keys[9], (D,), jnp.float32), 0.5, 1.5).astype(jnp.bfloat16),
        "norm1_bias": normal_values(arg_keys[10], (D,), 0.3, 2.0, ((0, 4),)),
        "norm2_gain": jnp.clip(1.0 + 0.1 * jax.random.normal(arg_keys[11], (D,), jnp.float32), 0.5, 1.5).astype(jnp.bfloat16),
        "norm2_bias": normal_values(arg_keys[12], (D,), 0.3, 2.0, ((0, 4),)),
        "router_weight": normal_values(arg_keys[13], (D, EXPERTS), (D // 4) ** -0.5, 0.4375, ((0, 4),)),
        "up_weight": normal_values(arg_keys[14], (EXPERTS, D, FF), D ** -0.5, 0.21875, ((0, 8),)),
        "up_bias": normal_values(arg_keys[15], (EXPERTS, FF), 0.5, 3.0, ((0, 8),)),
        "down_weight": normal_values(arg_keys[16], (EXPERTS, FF, D), (max(FF // 512, 1)) ** -0.5, 2.5, ((0, 8),)),
        "down_bias": normal_values(arg_keys[17], (EXPERTS, D), 2.0, 10.0, ((0, 8),)),
    }


epsilon = 1e-06
inv_root_two = 0.7071067811865476
inv_root_two_pi = 0.3989422804014327

def layer_norm(values, gain, shift):
    centred = values - lax.optimization_barrier(jnp.mean(values, axis=-1, keepdims=True))
    variance = lax.optimization_barrier(jnp.mean(centred * centred, axis=-1, keepdims=True))
    inv_std = lax.rsqrt(variance + epsilon)
    normed = centred * inv_std
    return (normed * gain.astype(jnp.float32) + shift.astype(jnp.float32), normed, inv_std)

def norm_backward(cotangent, normed, inv_std, gain):
    scaled = cotangent * gain.astype(jnp.float32)
    centred = scaled - lax.optimization_barrier(jnp.mean(scaled, axis=-1, keepdims=True)) - normed * lax.optimization_barrier(jnp.mean(scaled * normed, axis=-1, keepdims=True))
    return (centred * inv_std, lax.optimization_barrier(jnp.sum(cotangent * normed, axis=0)), lax.optimization_barrier(jnp.sum(cotangent, axis=0)))

def gelu_value(pre_act):
    return 0.5 * pre_act * (1.0 + jax.scipy.special.erf(pre_act * inv_root_two))

def gelu_slope(pre_act):
    cumulative = 0.5 * (1.0 + jax.scipy.special.erf(pre_act * inv_root_two))
    return cumulative + pre_act * jnp.exp(-0.5 * pre_act * pre_act) * inv_root_two_pi

def as_wide(values):
    return values.astype(jnp.float32)

def place_rows(pairs, flat_index, slot_total):
    model_width = pairs.shape[-1]
    empty = jnp.zeros((slot_total, model_width), pairs.dtype)
    return empty.at[flat_index.reshape(-1)].set(pairs.reshape(-1, model_width), mode='drop')

def gate_lookup(router_probs, chosen):
    labels = jnp.arange(router_probs.shape[1], dtype=jnp.int32)
    one_hot = (chosen[:, :, None] == labels[None, None, :]).astype(jnp.float32)
    return (lax.optimization_barrier(jnp.sum(router_probs[:, None, :] * one_hot, axis=-1)), one_hot)

def forward_block(block_rows, dense_full):
    qkv_full, q_shift, v_shift, out_full, out_shift, gain_one, shift_one, gain_two, shift_two, router_full = dense_full
    tok_rows = block_rows.shape[0]
    images = tok_rows // SEQ
    normed_in, normed_one, inv_one = layer_norm(block_rows, gain_one, shift_one)
    first_in = normed_in.astype(jnp.bfloat16)
    projected = jnp.dot(first_in, qkv_full, preferred_element_type=jnp.float32)
    queries = (projected[:, :D] + as_wide(q_shift)).astype(jnp.bfloat16).reshape(images, SEQ, HEADS, HEAD)
    key_heads = projected[:, D:2 * D].astype(jnp.bfloat16).reshape(images, SEQ, HEADS, HEAD)
    value_heads = (projected[:, 2 * D:] + as_wide(v_shift)).astype(jnp.bfloat16).reshape(images, SEQ, HEADS, HEAD)
    scores = jnp.einsum('bqhd,bkhd->bhqk', as_wide(queries), as_wide(key_heads)) * HEAD ** (-0.5)
    exp_scores = jnp.exp(scores)
    score_total = lax.optimization_barrier(jnp.sum(exp_scores, axis=-1, keepdims=True))
    log_total = jnp.log(score_total)
    attn_weights = (exp_scores / score_total).astype(jnp.bfloat16)
    attended = jnp.einsum('bhqk,bkhd->bqhd', as_wide(attn_weights), as_wide(value_heads)).astype(jnp.bfloat16).reshape(tok_rows, D)
    hidden = block_rows + jnp.dot(attended, out_full, preferred_element_type=jnp.float32) + as_wide(out_shift)
    normed_mid, normed_two, inv_two = layer_norm(hidden, gain_two, shift_two)
    second_in = normed_mid.astype(jnp.bfloat16)
    logits = jnp.dot(second_in, router_full, preferred_element_type=jnp.float32)
    router_exp = jnp.exp(logits)
    router_probs = router_exp / lax.optimization_barrier(jnp.sum(router_exp, axis=-1, keepdims=True))
    return (first_in, normed_one, inv_one, queries, key_heads, value_heads, log_total, attended, hidden, second_in, normed_two, inv_two, router_probs)

def backward_block(block_rows, cotangent, chosen, flat_index, expert_back, rows_back, dense_full):
    qkv_full, q_shift, v_shift, out_full, out_shift, gain_one, shift_one, gain_two, shift_two, router_full = dense_full
    kept = forward_block(block_rows, dense_full)
    first_in, normed_one, inv_one, queries, key_heads, value_heads, log_total, attended, hidden, second_in, normed_two, inv_two, router_probs = kept
    tok_rows = block_rows.shape[0]
    images = tok_rows // SEQ
    gate_values, one_hot = gate_lookup(router_probs, chosen)
    gathered_out = as_wide(jnp.take(expert_back, flat_index, axis=0, mode='fill', fill_value=0))
    block_out = hidden + lax.optimization_barrier(jnp.sum(gate_values[:, :, None] * gathered_out, axis=1))
    d_gates = lax.optimization_barrier(jnp.sum(cotangent[:, None, :] * gathered_out, axis=-1))
    d_probs = lax.optimization_barrier(jnp.sum(d_gates[:, :, None] * one_hot, axis=1))
    d_logits = (router_probs * (d_probs - lax.optimization_barrier(jnp.sum(router_probs * d_probs, axis=-1, keepdims=True)))).astype(jnp.bfloat16)
    router_grad = jnp.dot(second_in.T, d_logits, preferred_element_type=jnp.float32)
    row_grads = as_wide(jnp.take(rows_back, flat_index, axis=0, mode='fill', fill_value=0))
    d_second = jnp.dot(d_logits, router_full.T, preferred_element_type=jnp.float32) + lax.optimization_barrier(jnp.sum(row_grads, axis=1))
    d_mid, gain_two_grad, shift_two_grad = norm_backward(d_second, normed_two, inv_two, gain_two)
    d_hidden = cotangent + d_mid
    out_shift_grad = lax.optimization_barrier(jnp.sum(d_hidden, axis=0))
    d_hidden_b = d_hidden.astype(jnp.bfloat16)
    out_weight_grad = jnp.dot(attended.T, d_hidden_b, preferred_element_type=jnp.float32)
    d_attended = jnp.dot(d_hidden_b, out_full.T, preferred_element_type=jnp.float32).astype(jnp.bfloat16).reshape(images, SEQ, HEADS, HEAD)
    scores = jnp.einsum('bqhd,bkhd->bhqk', as_wide(queries), as_wide(key_heads)) * HEAD ** (-0.5)
    attn_again = jnp.exp(scores - log_total)
    attn_again_b = attn_again.astype(jnp.bfloat16)
    d_values = jnp.einsum('bhqk,bqhd->bkhd', as_wide(attn_again_b), as_wide(d_attended))
    d_att = jnp.einsum('bqhd,bkhd->bhqk', as_wide(d_attended), as_wide(value_heads))
    d_scores = (attn_again * (d_att - lax.optimization_barrier(jnp.sum(attn_again * d_att, axis=-1, keepdims=True))) * HEAD ** (-0.5)).astype(jnp.bfloat16)
    d_queries = jnp.einsum('bhqk,bkhd->bqhd', as_wide(d_scores), as_wide(key_heads))
    d_keys = jnp.einsum('bhqk,bqhd->bkhd', as_wide(d_scores), as_wide(queries))
    q_shift_grad = lax.optimization_barrier(jnp.sum(d_queries, axis=(0, 1))).reshape(D)
    v_shift_grad = lax.optimization_barrier(jnp.sum(d_values, axis=(0, 1))).reshape(D)
    d_projected = jnp.concatenate([d_queries.reshape(tok_rows, D), d_keys.reshape(tok_rows, D), d_values.reshape(tok_rows, D)], axis=1).astype(jnp.bfloat16)
    qkv_grad = jnp.dot(first_in.T, d_projected, preferred_element_type=jnp.float32)
    d_first = jnp.dot(d_projected, qkv_full.T, preferred_element_type=jnp.float32)
    d_input, gain_one_grad, shift_one_grad = norm_backward(d_first, normed_one, inv_one, gain_one)
    input_grad = d_hidden + d_input
    grads = (qkv_grad, q_shift_grad, v_shift_grad, out_weight_grad, out_shift_grad, gain_one_grad, shift_one_grad, gain_two_grad, shift_two_grad, router_grad)
    return (block_out, input_grad, grads)

def reference(block_in, out_grad, expert_ids, slot_ids, qkv_weight, q_bias, v_bias, out_weight, out_bias, norm1_gain, norm1_bias, norm2_gain, norm2_bias, router_weight, up_weight, up_bias, down_weight, down_bias):
    dense_full = (qkv_weight, q_bias, v_bias, out_weight, out_bias, norm1_gain, norm1_bias, norm2_gain, norm2_bias, router_weight)
    flat_all = jnp.where(slot_ids >= 0, expert_ids * CAP + slot_ids, EXPERTS * CAP).astype(jnp.int32)
    rows_in = block_in.reshape(DEVICES, TOK_DEV, D)
    rows_cot = out_grad.reshape(DEVICES, TOK_DEV, D)
    chosen_all = expert_ids.reshape(DEVICES, TOK_DEV, TOP)
    flat_blocks = flat_all.reshape(DEVICES, TOK_DEV, TOP)

    def front(carry, item):
        block_rows, cotangent, chosen, flat_index = item
        kept = forward_block(block_rows, dense_full)
        second_in, router_probs = (kept[9], kept[12])
        gate_values, one_hot = gate_lookup(router_probs, chosen)
        pairs = jnp.broadcast_to(second_in[:, None, :], (TOK_DEV, TOP, D))
        sent_rows = place_rows(pairs, flat_index, EXPERTS * CAP).reshape(EXPERTS, CAP, D)
        scaled = (gate_values[:, :, None] * cotangent[:, None, :]).astype(jnp.bfloat16)
        sent_grads = place_rows(scaled, flat_index, EXPERTS * CAP).reshape(EXPERTS, CAP, D)
        return (carry, (sent_rows, sent_grads))
    unused, stacked = lax.scan(front, jnp.zeros((), jnp.float32), (rows_in, rows_cot, chosen_all, flat_blocks))
    dispatched = jnp.swapaxes(stacked[0], 0, 1)
    grad_rows = jnp.swapaxes(stacked[1], 0, 1)

    def expert_pass(item):
        up_full, up_shift, down_full, down_shift, inputs_e, grads_e = item
        row_block = inputs_e.reshape(DEVICES * CAP, D)
        grad_block = grads_e.reshape(DEVICES * CAP, D)
        pre_act = jnp.dot(row_block, up_full, preferred_element_type=jnp.float32) + as_wide(up_shift)
        active = gelu_value(pre_act).astype(jnp.bfloat16)
        expert_out = (jnp.dot(active, down_full, preferred_element_type=jnp.float32) + as_wide(down_shift)).astype(jnp.bfloat16)
        down_grad = jnp.dot(active.T, grad_block, preferred_element_type=jnp.float32)
        down_shift_grad = lax.optimization_barrier(jnp.sum(as_wide(grad_block), axis=0))
        d_pre = jnp.dot(grad_block, down_full.T, preferred_element_type=jnp.float32) * gelu_slope(pre_act)
        d_pre_b = d_pre.astype(jnp.bfloat16)
        up_grad = jnp.dot(row_block.T, d_pre_b, preferred_element_type=jnp.float32)
        up_shift_grad = lax.optimization_barrier(jnp.sum(d_pre, axis=0))
        d_rows = jnp.dot(d_pre_b, up_full.T, preferred_element_type=jnp.float32).astype(jnp.bfloat16)
        return (expert_out.reshape(DEVICES, CAP, D), d_rows.reshape(DEVICES, CAP, D), up_grad, up_shift_grad, down_grad, down_shift_grad)
    expert_results = lax.map(expert_pass, (up_weight, up_bias, down_weight, down_bias, dispatched, grad_rows))
    outs_back = jnp.swapaxes(expert_results[0], 0, 1).reshape(DEVICES, EXPERTS * CAP, D)
    rows_back = jnp.swapaxes(expert_results[1], 0, 1).reshape(DEVICES, EXPERTS * CAP, D)

    def back(totals, item):
        block_rows, cotangent, chosen, flat_index, expert_back, grads_back = item
        block_out, input_grad, grads = backward_block(block_rows, cotangent, chosen, flat_index, expert_back, grads_back, dense_full)
        return (jax.tree.map(jnp.add, totals, grads), (block_out, input_grad))
    initial = (jnp.zeros((D, 3 * D), jnp.float32), jnp.zeros((D,), jnp.float32), jnp.zeros((D,), jnp.float32), jnp.zeros((D, D), jnp.float32), jnp.zeros((D,), jnp.float32), jnp.zeros((D,), jnp.float32), jnp.zeros((D,), jnp.float32), jnp.zeros((D,), jnp.float32), jnp.zeros((D,), jnp.float32), jnp.zeros((D, EXPERTS), jnp.float32))
    final, per_block = lax.scan(back, initial, (rows_in, rows_cot, chosen_all, flat_blocks, outs_back, rows_back))
    block_out = per_block[0].reshape(TOKENS, D)
    input_grad = per_block[1].reshape(TOKENS, D)
    return (block_out, input_grad, final[0], final[1], final[2], final[3], final[4], final[5], final[6], final[7], final[8], final[9], expert_results[2], expert_results[3], expert_results[4], expert_results[5])
```

```python
import jax
import jax.numpy as jnp
from jax import lax
from jax.sharding import Mesh, PartitionSpec as P

HEADS = 12
HEAD = 64
SEQ = 197

epsilon = 1e-06
inv_root_two = 0.7071067811865476
inv_root_two_pi = 0.3989422804014327

bf16 = jnp.bfloat16
f32 = jnp.float32


def layer_norm(values, gain, shift):
    centred = values - jnp.mean(values, axis=-1, keepdims=True)
    variance = jnp.mean(centred * centred, axis=-1, keepdims=True)
    inv_std = lax.rsqrt(variance + epsilon)
    normed = centred * inv_std
    return (normed * gain + shift, normed, inv_std)


def norm_backward(cotangent, normed, inv_std, gain):
    scaled = cotangent * gain
    centred = (
        scaled
        - jnp.mean(scaled, axis=-1, keepdims=True)
        - normed * jnp.mean(scaled * normed, axis=-1, keepdims=True)
    )
    return (centred * inv_std, jnp.sum(cotangent * normed, axis=0), jnp.sum(cotangent, axis=0))


def gelu_value(pre_act):
    return 0.5 * pre_act * (1.0 + lax.erf(pre_act * inv_root_two))


def gelu_slope(pre_act):
    cumulative = 0.5 * (1.0 + lax.erf(pre_act * inv_root_two))
    return cumulative + pre_act * jnp.exp(-0.5 * pre_act * pre_act) * inv_root_two_pi


def dot(a, b):
    return jnp.dot(a, b, preferred_element_type=f32)


def dot_tn(a, b):
    return lax.dot_general(a, b, (((0,), (0,)), ((), ())), preferred_element_type=f32)


def dot_nt(a, b):
    return lax.dot_general(a, b, (((1,), (1,)), ((), ())), preferred_element_type=f32)


def shift_along(value, axis, step):
    size = lax.axis_size(axis)
    return lax.ppermute(value, axis, [(i, (i + step) % size) for i in range(size)])


def pick(value, index, axis):
    return lax.dynamic_index_in_dim(value, index, axis, keepdims=False)


def expert_grad_sum(total):
    outer, fan = lax.axis_size("hi"), lax.axis_size("lo")
    high, low = lax.axis_index("hi"), lax.axis_index("lo")
    rows, columns = total.shape
    blocks = total.reshape(outer, fan, rows // (outer * fan), columns)
    mine = [None] * fan
    for step in list(range(1, fan)) + [0]:
        piece = pick(blocks, (low + step) % fan, 1)
        summed = pick(piece, high, 0)
        for hop in range(1, outer):
            sent = pick(piece, (high + hop) % outer, 0).astype(bf16)
            summed = summed + shift_along(sent, "hi", hop).astype(f32)
        if step:
            summed = shift_along(summed.astype(bf16), "lo", step).astype(f32)
        mine[step] = summed
    if fan == 2:
        first = jnp.where(low == 0, mine[0], mine[1])
        second = jnp.where(low == 0, mine[1], mine[0])
        return jnp.stack([first, second])
    stacked = jnp.stack(mine)
    return jnp.stack([pick(stacked, (low - k) % fan, 0) for k in range(fan)])


def gather_small(vector):
    names = ("hi", "lo")
    size = lax.axis_size("hi") * lax.axis_size("lo")
    me = lax.axis_index("hi") * lax.axis_size("lo") + lax.axis_index("lo")
    rows = [vector]
    for step in range(1, size):
        rows.append(lax.ppermute(vector, names, [(i, (i + step) % size) for i in range(size)]))
    return jnp.stack(rows), me


def dense_sum(matrix):
    names = ("hi", "lo")
    members = lax.axis_size("hi") * lax.axis_size("lo")
    me = lax.axis_index("hi") * lax.axis_size("lo") + lax.axis_index("lo")
    plane = lax.axis_size("expert")
    spot = lax.axis_index("expert")
    rows, columns = matrix.shape
    piece = rows // (members * plane)
    current = matrix.reshape(members, plane, piece, columns)
    left, bit = plane, 1
    while left > 1:
        halves = current.reshape(members, left // 2, 2, piece, columns)
        side = (spot // bit) % 2
        sent = pick(halves, 1 - side, 2).astype(bf16)
        came = lax.ppermute(sent, "expert", [(i, i ^ bit) for i in range(plane)])
        current = pick(halves, side, 2) + came.astype(f32)
        left //= 2
        bit *= 2
    current = current.reshape(members, piece, columns)
    summed = pick(current, me, 0)
    for step in range(1, members):
        sent = pick(current, (me + step) % members, 0).astype(bf16)
        came = lax.ppermute(sent, names, [(i, (i + step) % members) for i in range(members)])
        summed = summed + came.astype(f32)
    return summed


def local(
    block_in,
    out_grad,
    expert_ids,
    slot_ids,
    qkv_weight,
    q_bias,
    v_bias,
    out_weight,
    out_bias,
    norm1_gain,
    norm1_bias,
    norm2_gain,
    norm2_bias,
    router_weight,
    up_weight,
    up_bias,
    down_weight,
    down_bias,
):
    tok_rows, width = block_in.shape
    images = tok_rows // SEQ
    experts = router_weight.shape[1]
    capacity = tok_rows * 2 * 9 // (8 * experts) + 1
    slots = -(-capacity // 16) * 16
    outer, fan, plane = lax.axis_size("hi"), lax.axis_size("lo"), lax.axis_size("expert")
    members = outer * fan
    low, spot = lax.axis_index("lo"), lax.axis_index("expert")
    me = lax.axis_index("hi") * fan + low
    group = ("lo", "expert")
    hidden_width = up_weight.shape[2]
    head_scale = HEAD ** (-0.5)

    vectors = (q_bias, v_bias, out_bias, norm1_gain, norm1_bias, norm2_gain, norm2_bias)
    packed = jnp.concatenate([qkv_weight, out_weight, router_weight] + [v[:, None] for v in vectors], axis=1)
    part = packed.shape[0] // plane
    packed = lax.dynamic_slice_in_dim(packed, spot * part, part, 0)
    packed = lax.all_gather(packed, ("hi", "lo", "expert"), axis=0, tiled=True)
    qkv_full = packed[:, : 3 * width]
    out_full = packed[:, 3 * width : 4 * width]
    router_full = packed[:, 4 * width : 4 * width + experts]
    rows = packed[:, 4 * width + experts :].T.astype(f32)
    q_shift, v_shift, out_shift, gain_one, shift_one, gain_two, shift_two = [rows[i] for i in range(7)]

    up_one = pick(up_weight, low, 0)
    down_one = pick(down_weight, low, 0)
    up_shift = pick(up_bias, low, 0).astype(f32)
    down_shift = pick(down_bias, low, 0).astype(f32)

    owner = (expert_ids % fan) * plane + expert_ids // fan
    spots = jnp.where(slot_ids >= 0, owner * slots + slot_ids, -1)
    total = experts * slots
    labels = jnp.arange(total, dtype=jnp.int32)
    place = ((labels[:, None] == spots[:, 0][None, :]) | (labels[:, None] == spots[:, 1][None, :])).astype(bf16)

    def exchange(value):
        return lax.all_to_all(value, group, split_axis=0, concat_axis=0, tiled=True)

    cot_rows = exchange(dot(place, out_grad.astype(bf16)).astype(bf16))

    normed_in, normed_one, inv_one = layer_norm(block_in, gain_one, shift_one)
    first_in = normed_in.astype(bf16)
    projected = dot(first_in, qkv_full)
    queries = (projected[:, :width] + q_shift).astype(bf16).reshape(images, SEQ, HEADS, HEAD)
    key_heads = projected[:, width : 2 * width].astype(bf16).reshape(images, SEQ, HEADS, HEAD)
    value_heads = (projected[:, 2 * width :] + v_shift).astype(bf16).reshape(images, SEQ, HEADS, HEAD)
    scores = jnp.einsum("bqhd,bkhd->bhqk", queries, key_heads, preferred_element_type=f32) * head_scale
    exp_scores = jnp.exp(scores)
    score_total = jnp.sum(exp_scores, axis=-1, keepdims=True)
    log_total = jnp.log(score_total)
    attn_weights = (exp_scores / score_total).astype(bf16)
    attended = (
        jnp.einsum("bhqk,bkhd->bqhd", attn_weights, value_heads, preferred_element_type=f32)
        .astype(bf16)
        .reshape(tok_rows, width)
    )
    hidden = block_in + dot(attended, out_full) + out_shift
    normed_mid, normed_two, inv_two = layer_norm(hidden, gain_two, shift_two)
    second_in = normed_mid.astype(bf16)
    logits = dot(second_in, router_full)
    router_exp = jnp.exp(logits)
    router_probs = router_exp / jnp.sum(router_exp, axis=-1, keepdims=True)
    one_hot = (expert_ids[:, :, None] == jnp.arange(experts, dtype=jnp.int32)[None, None, :]).astype(f32)
    gate_values = jnp.sum(router_probs[:, None, :] * one_hot, axis=-1)

    row_recv = exchange(dot(place, second_in).astype(bf16))

    row_exp = jnp.exp(dot(row_recv, router_full))
    mine = (jnp.arange(experts, dtype=jnp.int32) == spot * fan + low).astype(f32)
    row_gate = jnp.sum(row_exp * mine, axis=-1) / jnp.sum(row_exp, axis=-1)
    grad_recv = (row_gate[:, None] * cot_rows.astype(f32)).astype(bf16)
    pre_act = dot(row_recv, up_one) + up_shift
    active = gelu_value(pre_act).astype(bf16)
    down_grad = dot_tn(active, grad_recv)
    down_part = expert_grad_sum(down_grad)
    d_pre = dot_nt(grad_recv, down_one) * gelu_slope(pre_act)
    d_pre_b = d_pre.astype(bf16)
    up_grad = dot_tn(row_recv, d_pre_b)
    up_part = expert_grad_sum(up_grad)
    outs_back = exchange((dot(active, down_one) + down_shift).astype(bf16))
    rows_back = exchange(dot_nt(d_pre_b, up_one).astype(bf16))
    small, me = gather_small(
        jnp.concatenate([jnp.sum(d_pre, axis=0), jnp.sum(grad_recv.astype(f32), axis=0)])
    )
    from_expert = (me - jnp.arange(members)) % fan
    small = jnp.stack([jnp.sum(jnp.where((from_expert == k)[:, None], small, 0.0), axis=0) for k in range(fan)])
    up_shift_part = lax.dynamic_slice_in_dim(
        small[:, :hidden_width], me * (hidden_width // members), hidden_width // members, 1
    )
    down_shift_part = lax.dynamic_slice_in_dim(small[:, hidden_width:], me * (width // members), width // members, 1)

    take0 = (spots[:, 0][:, None] == labels[None, :]).astype(bf16)
    take1 = (spots[:, 1][:, None] == labels[None, :]).astype(bf16)
    got0, got1 = dot(take0, outs_back), dot(take1, outs_back)
    block_out = hidden + gate_values[:, :1] * got0 + gate_values[:, 1:] * got1
    d_gates = jnp.stack([jnp.sum(out_grad * got0, axis=-1), jnp.sum(out_grad * got1, axis=-1)], axis=1)
    d_probs = jnp.sum(d_gates[:, :, None] * one_hot, axis=1)
    d_logits = (router_probs * (d_probs - jnp.sum(router_probs * d_probs, axis=-1, keepdims=True))).astype(bf16)
    router_grad = dot_tn(second_in, d_logits)
    d_second = dot_nt(d_logits, router_full) + dot(take0 + take1, rows_back)
    d_mid, gain_two_grad, shift_two_grad = norm_backward(d_second, normed_two, inv_two, gain_two)
    d_hidden = out_grad + d_mid
    out_shift_grad = jnp.sum(d_hidden, axis=0)
    d_hidden_b = d_hidden.astype(bf16)
    out_weight_grad = dot_tn(attended, d_hidden_b)
    d_attended = dot_nt(d_hidden_b, out_full).astype(bf16).reshape(images, SEQ, HEADS, HEAD)
    scores_again = jnp.einsum("bqhd,bkhd->bhqk", queries, key_heads, preferred_element_type=f32) * head_scale
    attn_again = jnp.exp(scores_again - log_total)
    attn_again_b = attn_again.astype(bf16)
    d_values = jnp.einsum("bhqk,bqhd->bkhd", attn_again_b, d_attended, preferred_element_type=f32)
    d_att = jnp.einsum("bqhd,bkhd->bhqk", d_attended, value_heads, preferred_element_type=f32)
    d_scores = (
        attn_again * (d_att - jnp.sum(attn_again * d_att, axis=-1, keepdims=True)) * head_scale
    ).astype(bf16)
    d_queries = jnp.einsum("bhqk,bkhd->bqhd", d_scores, key_heads, preferred_element_type=f32)
    d_keys = jnp.einsum("bhqk,bqhd->bkhd", d_scores, queries, preferred_element_type=f32)
    q_shift_grad = jnp.sum(d_queries, axis=(0, 1)).reshape(width)
    v_shift_grad = jnp.sum(d_values, axis=(0, 1)).reshape(width)
    d_projected = jnp.concatenate(
        [d.reshape(tok_rows, width) for d in (d_queries, d_keys, d_values)], axis=1
    ).astype(bf16)
    qkv_grad = dot_tn(first_in, d_projected)
    d_first = dot_nt(d_projected, qkv_full)
    d_input, gain_one_grad, shift_one_grad = norm_backward(d_first, normed_one, inv_one, gain_one)
    input_grad = d_hidden + d_input

    columns = (q_shift_grad, v_shift_grad, out_shift_grad, gain_one_grad, shift_one_grad, gain_two_grad, shift_two_grad)
    dense = dense_sum(
        jnp.concatenate([qkv_grad, out_weight_grad, router_grad, jnp.stack(columns, axis=1)], axis=1)
    )
    vec = 4 * width + experts
    return (
        block_out,
        input_grad,
        dense[:, : 3 * width],
        dense[:, vec],
        dense[:, vec + 1],
        dense[:, 3 * width : 4 * width],
        dense[:, vec + 2],
        dense[:, vec + 3],
        dense[:, vec + 4],
        dense[:, vec + 5],
        dense[:, vec + 6],
        dense[:, 4 * width : vec],
        up_part,
        up_shift_part,
        down_part,
        down_shift_part,
    )


def solution(mesh):
    def step(*arrays):
        members, plane = mesh.shape["dp"], mesh.shape["expert"]
        fan = arrays[14].shape[0] // plane
        split = Mesh(mesh.devices.reshape(members // fan, fan, plane), ("hi", "lo", "expert"))
        every, dp = ("hi", "lo", "expert"), ("hi", "lo")
        in_specs = (
            (P(every, None),) * 4
            + (P(dp, None), P(dp), P(dp), P(dp, None), P(dp), P(dp), P(dp), P(dp), P(dp), P(dp, None))
            + (P("expert", None, None), P("expert", None), P("expert", None, None), P("expert", None))
        )
        out_specs = (
            (P(every, None),) * 3
            + (P(every), P(every), P(every, None))
            + (P(every),) * 5
            + (P(every, None), P("expert", dp, None), P("expert", dp), P("expert", dp, None), P("expert", dp))
        )
        return jax.shard_map(local, mesh=split, in_specs=in_specs, out_specs=out_specs, check_vma=False)(*arrays)

    return step
```

```python
import functools

import jax
import jax.numpy as jnp
from jax import lax
from jax.experimental import pallas as pl
from jax.experimental.pallas import tpu as pltpu
from jax.sharding import Mesh, PartitionSpec as P


HEAD = 64
SEQ = 197

epsilon = 1e-06
inv_root_two = 0.7071067811865476
inv_root_two_pi = 0.3989422804014327

bf16 = jnp.bfloat16
f32 = jnp.float32
LANES = 128
SEQ_PAD = -(-SEQ // 16) * 16
ROW_TILE = 64
head_scale = HEAD ** (-0.5)
VMEM_MAX = 60 * 1024 * 1024


def dot(a, b):
    return jnp.dot(a, b, preferred_element_type=f32)


def dot_tn(a, b):
    return lax.dot_general(a, b, (((0,), (0,)), ((), ())), preferred_element_type=f32)


def dot_nt(a, b):
    return lax.dot_general(a, b, (((1,), (1,)), ((), ())), preferred_element_type=f32)


def iota(shape, axis):
    return lax.broadcasted_iota(jnp.int32, shape, axis)


def row_valid(start, count):
    return (iota((count, 1), 0) + start) % SEQ_PAD < SEQ


def normed_rows(values):
    centred = values - jnp.mean(values, axis=-1, keepdims=True)
    inv_std = lax.rsqrt(jnp.mean(centred * centred, axis=-1, keepdims=True) + epsilon)
    return centred * inv_std, inv_std


def norm_row_grad(scaled, normed, inv_std):
    return (
        scaled
        - jnp.mean(scaled, axis=-1, keepdims=True)
        - normed * jnp.mean(scaled * normed, axis=-1, keepdims=True)
    ) * inv_std


def tile_of(index, size):
    return pl.ds(pl.multiple_of(index * size, size), size)


def front_kernel(
    experts, x_ref, w_ref, small_ref, bias_ref, vec_ref, spots_ref,
    qkv_ref, att_ref, hid_ref, sec_ref, probs_ref, send_ref, first_ref,
):
    rows, width = x_ref.shape
    col = 256
    gain_one, shift_one = vec_ref[3:4, :], vec_ref[4:5, :]
    gain_two, shift_two = vec_ref[5:6, :], vec_ref[6:7, :]

    @pl.loop(0, rows // ROW_TILE)
    def _(t):
        at = tile_of(t, ROW_TILE)
        normed, _ = normed_rows(x_ref[at, :])
        first_ref[at, :] = (normed * gain_one + shift_one).astype(bf16)

    valid = row_valid(0, rows)

    @pl.loop(0, 3 * width // col)
    def _(j):
        at = tile_of(j, col)
        got = dot(first_ref[...], w_ref[:, at]) + bias_ref[:, at]
        qkv_ref[:, at] = jnp.where(valid, got, 0.0).astype(bf16)

    low = iota((1, LANES), 1) < HEAD
    keys = iota((1, SEQ_PAD), 1) < SEQ
    pairs = width // LANES

    @pl.loop(0, (rows // SEQ_PAD) * pairs)
    def _(n):
        at = tile_of(n // pairs, SEQ_PAD)
        lane = (n % pairs) * LANES
        q = qkv_ref[at, pl.ds(pl.multiple_of(lane, LANES), LANES)]
        k = qkv_ref[at, pl.ds(pl.multiple_of(width + lane, LANES), LANES)]
        v = qkv_ref[at, pl.ds(pl.multiple_of(2 * width + lane, LANES), LANES)]
        parts = []
        for side in (low, ~low):
            scores = dot_nt(jnp.where(side, q, jnp.zeros_like(q)), k) * head_scale
            weights = jnp.where(keys, jnp.exp(scores), 0.0)
            weights = weights * (1.0 / jnp.sum(weights, axis=-1, keepdims=True))
            parts.append(dot(weights.astype(bf16), v))
        att_ref[at, pl.ds(pl.multiple_of(lane, LANES), LANES)] = jnp.where(low, *parts).astype(bf16)

    @pl.loop(0, width // col)
    def _(j):
        at = tile_of(j, col)
        wide = pl.ds(pl.multiple_of(3 * width + j * col, col), col)
        hid_ref[:, at] = x_ref[:, at] + dot(att_ref[...], w_ref[:, wide]) + vec_ref[2:3, at]

    lanes = iota((1, LANES), 1) < experts

    @pl.loop(0, rows // ROW_TILE)
    def _(t):
        at = tile_of(t, ROW_TILE)
        normed, _ = normed_rows(hid_ref[at, :])
        ok = row_valid(t * ROW_TILE, ROW_TILE)
        second = jnp.where(ok, normed * gain_two + shift_two, 0.0).astype(bf16)
        sec_ref[at, :] = second
        grown = jnp.where(lanes, jnp.exp(jnp.where(lanes, dot(second, small_ref[...]), 0.0)), 0.0)
        probs_ref[at, :] = grown / jnp.sum(grown, axis=-1, keepdims=True)

    place_rows(spots_ref, sec_ref, send_ref)


def place_rows(spots_ref, rows_ref, send_ref):
    total, rows = send_ref.shape[0], rows_ref.shape[0]
    block = total // 4

    @pl.loop(0, 4)
    def _(d):
        labels = iota((block, rows), 0) + d * block
        hit = (labels == spots_ref[0:1, :]) | (labels == spots_ref[1:2, :])
        send_ref[tile_of(d, block), :] = dot(jnp.where(hit, 1.0, 0.0).astype(bf16), rows_ref[...]).astype(bf16)


def place_kernel(spots_ref, rows_ref, send_ref, held_ref):
    held_ref[...] = rows_ref[...].astype(bf16)
    place_rows(spots_ref, held_ref, send_ref)


def whole(n):
    return [pl.BlockSpec(memory_space=pltpu.VMEM)] * n


def params(**more):
    return pltpu.CompilerParams(vmem_limit_bytes=VMEM_MAX, **more)


def place_call(spots, values, total):
    rows, width = values.shape
    return pl.pallas_call(
        place_kernel,
        out_shape=jax.ShapeDtypeStruct((total, width), bf16),
        in_specs=whole(2),
        out_specs=whole(1)[0],
        scratch_shapes=[pltpu.VMEM((rows, width), bf16)],
        compiler_params=params(),
        cost_estimate=pl.CostEstimate(flops=2 * total * rows * width, bytes_accessed=rows * width * 4 + total * width * 2, transcendentals=0),
        name="place",
    )(spots, values)


def front_call(experts, total, x, weights, small, bias, vec, spots):
    rows, width = x.shape
    shapes = (
        jax.ShapeDtypeStruct((rows, 3 * width), bf16),
        jax.ShapeDtypeStruct((rows, width), bf16),
        jax.ShapeDtypeStruct((rows, width), f32),
        jax.ShapeDtypeStruct((rows, width), bf16),
        jax.ShapeDtypeStruct((rows, LANES), f32),
        jax.ShapeDtypeStruct((total, width), bf16),
    )
    return pl.pallas_call(
        functools.partial(front_kernel, experts),
        out_shape=shapes,
        in_specs=whole(6),
        out_specs=tuple(whole(6)),
        scratch_shapes=[pltpu.VMEM((rows, width), bf16)],
        compiler_params=params(),
        cost_estimate=pl.CostEstimate(flops=14 * 10**9, bytes_accessed=30 * 10**6, transcendentals=2 * 10**6),
        name="front",
    )(x, weights, small, bias, vec, spots)


def gelu_parts(pre_act):
    cumulative = 0.5 * (1.0 + lax.erf(pre_act * inv_root_two))
    return pre_act * cumulative, cumulative


def gate_kernel(experts, which_ref, x_ref, cot_ref, small_ref, grad_ref, sum_ref):
    lane = iota((1, LANES), 1)
    mine = lane == which_ref[0]
    total = jnp.zeros((1, cot_ref.shape[1]), f32)
    rows = x_ref.shape[0]
    size = 128

    def step(t, total):
        at = tile_of(t, size)
        logits = jnp.where(lane < experts, dot(x_ref[at, :], small_ref[...]), 0.0)
        grown = jnp.where(lane < experts, jnp.exp(logits), 0.0)
        gate = jnp.sum(jnp.where(mine, grown, 0.0), axis=-1, keepdims=True) / jnp.sum(grown, axis=-1, keepdims=True)
        scaled = (gate * cot_ref[at, :].astype(f32)).astype(bf16)
        grad_ref[at, :] = scaled
        return total + jnp.sum(scaled.astype(f32), axis=0, keepdims=True)

    sum_ref[...] = lax.fori_loop(0, rows // size, step, total)


def gate_call(experts, which, rows_in, cot, small):
    return pl.pallas_call(
        functools.partial(gate_kernel, experts),
        out_shape=(jax.ShapeDtypeStruct(cot.shape, bf16), jax.ShapeDtypeStruct((1, cot.shape[1]), f32)),
        in_specs=[pl.BlockSpec(memory_space=pltpu.SMEM)] + whole(3),
        out_specs=tuple(whole(2)),
        compiler_params=params(),
        cost_estimate=pl.CostEstimate(flops=10**9, bytes_accessed=3 * cot.size * 2, transcendentals=10**5),
        name="gate",
    )(which, rows_in, cot, small)


def down_kernel(x_ref, grad_ref, up_ref, shift_ref, out_ref, act_ref):
    rows = x_ref.shape[0]
    size = rows // 4

    @pl.loop(0, 4)
    def _(t):
        at = tile_of(t, size)
        act_ref[at, :] = gelu_parts(dot(x_ref[at, :], up_ref[...]) + shift_ref[...])[0].astype(bf16)

    out_ref[...] = dot_tn(act_ref[...], grad_ref[...]).astype(bf16)


def down_call(x, grads, up, shift, tile, part, parts):
    rows, width = x.shape
    span = up.shape[1] // parts
    steps = span // tile
    grid = pltpu.PrefetchScalarGridSpec(
        num_scalar_prefetch=1,
        grid=(steps,),
        in_specs=[
            pl.BlockSpec((rows, width), lambda j, p: (0, 0)),
            pl.BlockSpec((rows, width), lambda j, p: (0, 0)),
            pl.BlockSpec((width, tile), lambda j, p: (0, p[0] * steps + j)),
            pl.BlockSpec((1, tile), lambda j, p: (0, p[0] * steps + j)),
        ],
        out_specs=pl.BlockSpec((tile, width), lambda j, p: (j, 0)),
        scratch_shapes=[pltpu.VMEM((rows, tile), bf16)],
    )
    return pl.pallas_call(
        lambda p_ref, *refs: down_kernel(*refs),
        out_shape=jax.ShapeDtypeStruct((span, width), bf16),
        grid_spec=grid,
        compiler_params=params(dimension_semantics=("arbitrary",)),
        cost_estimate=pl.CostEstimate(flops=4 * rows * width * span, bytes_accessed=4 * rows * width + 4 * span * width, transcendentals=rows * span),
        name="down",
    )(part, x, grads, up, shift)


def expert_kernel(
    x_ref, grad_ref, up_ref, shift_ref, down_ref, down_shift_ref,
    upg_ref, upsum_ref, out_ref, rows_ref, pre_ref, dpre_ref, out_acc, rows_acc,
):
    j = pl.program_id(0)
    rows, _ = x_ref.shape
    tile = up_ref.shape[1]
    size = rows // 4

    @pl.when(j == 0)
    def _():
        out_acc[...] = jnp.broadcast_to(down_shift_ref[...], out_acc.shape)
        rows_acc[...] = jnp.zeros_like(rows_acc)

    def step(t, total):
        at = tile_of(t, size)
        pre = dot(x_ref[at, :], up_ref[...]) + shift_ref[...]
        act, cumulative = gelu_parts(pre)
        slope = cumulative + pre * jnp.exp(-0.5 * pre * pre) * inv_root_two_pi
        d_pre = dot_nt(grad_ref[at, :], down_ref[...]) * slope
        d_pre_b = d_pre.astype(bf16)
        dpre_ref[at, :] = d_pre_b
        out_acc[at, :] += dot(act.astype(bf16), down_ref[...])
        rows_acc[at, :] += dot_nt(d_pre_b, up_ref[...])
        return total + jnp.sum(d_pre, axis=0, keepdims=True)

    upsum_ref[...] = lax.fori_loop(0, 4, step, jnp.zeros((1, tile), f32))
    upg_ref[...] = dot_tn(x_ref[...], dpre_ref[...]).astype(bf16)

    @pl.when(j == pl.num_programs(0) - 1)
    def _():
        out_ref[...] = out_acc[...].astype(bf16)
        rows_ref[...] = rows_acc[...].astype(bf16)


def expert_call(x, grads, up, shift, down, down_shift, tile):
    rows, width = x.shape
    hidden = up.shape[1]
    fixed = lambda *shape: pl.BlockSpec(shape, lambda j: (0, 0))
    return pl.pallas_call(
        expert_kernel,
        out_shape=(
            jax.ShapeDtypeStruct((width, hidden), bf16),
            jax.ShapeDtypeStruct((1, hidden), f32),
            jax.ShapeDtypeStruct((rows, width), bf16),
            jax.ShapeDtypeStruct((rows, width), bf16),
        ),
        grid=(hidden // tile,),
        in_specs=[
            fixed(rows, width),
            fixed(rows, width),
            pl.BlockSpec((width, tile), lambda j: (0, j)),
            pl.BlockSpec((1, tile), lambda j: (0, j)),
            pl.BlockSpec((tile, width), lambda j: (j, 0)),
            fixed(1, width),
        ],
        out_specs=(
            pl.BlockSpec((width, tile), lambda j: (0, j)),
            pl.BlockSpec((1, tile), lambda j: (0, j)),
            fixed(rows, width),
            fixed(rows, width),
        ),
        scratch_shapes=[
            pltpu.VMEM((8, LANES), f32),
            pltpu.VMEM((rows, tile), bf16),
            pltpu.VMEM((rows, width), f32),
            pltpu.VMEM((rows, width), f32),
        ],
        compiler_params=params(dimension_semantics=("arbitrary",)),
        cost_estimate=pl.CostEstimate(flops=10 * rows * width * hidden, bytes_accessed=8 * rows * width + 6 * hidden * width, transcendentals=2 * rows * hidden),
        name="expert",
    )(x, grads, up, shift, down, down_shift)


def combine_kernel(
    outs_ref, back_ref, cot_ref, hid_ref, sec_ref, probs_ref, spots_ref, ids_ref, w_ref, small_ref, vec_ref,
    blk_ref, dhid_ref, dhb_ref, datt_ref, dlog_ref, sums_ref,
):
    rows, width = cot_ref.shape
    total = outs_ref.shape[0]
    size = SEQ_PAD
    gain_two = vec_ref[5:6, :]
    labels = iota((1, total), 1)
    lane = iota((1, LANES), 1)

    def step(t, sums):
        at = tile_of(t, size)
        first = jnp.where(spots_ref[at, 0:1] == labels, 1.0, 0.0).astype(bf16)
        second = jnp.where(spots_ref[at, 1:2] == labels, 1.0, 0.0).astype(bf16)
        got0, got1 = dot(first, outs_ref[...]), dot(second, outs_ref[...])
        back = dot(first + second, back_ref[...])
        probs = probs_ref[at, :]
        hot0 = jnp.where(ids_ref[at, 0:1] == lane, 1.0, 0.0)
        hot1 = jnp.where(ids_ref[at, 1:2] == lane, 1.0, 0.0)
        gate0 = jnp.sum(probs * hot0, axis=-1, keepdims=True)
        gate1 = jnp.sum(probs * hot1, axis=-1, keepdims=True)
        cot = cot_ref[at, :]
        hid = hid_ref[at, :]
        blk_ref[at, :] = hid + gate0 * got0 + gate1 * got1
        d0 = jnp.sum(cot * got0, axis=-1, keepdims=True)
        d1 = jnp.sum(cot * got1, axis=-1, keepdims=True)
        d_probs = d0 * hot0 + d1 * hot1
        d_logits = (probs * (d_probs - jnp.sum(probs * d_probs, axis=-1, keepdims=True))).astype(bf16)
        dlog_ref[at, :] = d_logits
        d_second = dot_nt(d_logits, small_ref[...]) + back
        normed, inv_std = normed_rows(hid)
        d_hidden = cot + norm_row_grad(d_second * gain_two, normed, inv_std)
        dhid_ref[at, :] = d_hidden
        d_hidden_b = d_hidden.astype(bf16)
        dhb_ref[at, :] = d_hidden_b
        datt_ref[at, :] = dot_nt(d_hidden_b, w_ref[...]).astype(bf16)
        add = lambda v: jnp.sum(v, axis=0, keepdims=True)
        return tuple(s + add(v) for s, v in zip(sums, (d_hidden, d_second * normed, d_second)))

    zero = jnp.zeros((1, width), f32)
    sums = lax.fori_loop(0, rows // size, step, (zero, zero, zero))
    for i, s in enumerate(sums):
        sums_ref[i : i + 1, :] = s


def combine_call(outs, back, cot, hid, sec, probs, spots, ids, weights, small, vec):
    rows, width = cot.shape
    shapes = (
        jax.ShapeDtypeStruct((rows, width), f32),
        jax.ShapeDtypeStruct((rows, width), f32),
        jax.ShapeDtypeStruct((rows, width), bf16),
        jax.ShapeDtypeStruct((rows, width), bf16),
        jax.ShapeDtypeStruct((rows, LANES), bf16),
        jax.ShapeDtypeStruct((8, width), f32),
    )
    return pl.pallas_call(
        combine_kernel,
        out_shape=shapes,
        grid=(1,),
        in_specs=[
            *[pl.BlockSpec(a.shape, lambda i: (0, 0)) for a in (outs, back, cot, hid, sec, probs, spots, ids)],
            pl.BlockSpec((width, width), lambda i: (0, 3)),
            *[pl.BlockSpec(a.shape, lambda i: (0, 0)) for a in (small, vec)],
        ],
        out_specs=tuple(pl.BlockSpec(s.shape, lambda i: (0, 0)) for s in shapes),
        compiler_params=params(),
        cost_estimate=pl.CostEstimate(flops=8 * 10**9, bytes_accessed=25 * 10**6, transcendentals=0),
        name="combine",
    )(outs, back, cot, hid, sec, probs, spots, ids, weights, small, vec)


def back_kernel(
    experts, x_ref, qkv_ref, datt_ref, dhid_ref, dhb_ref, att_ref, sec_ref, dlog_ref, w_ref, vec_ref, sums_ref,
    in_ref, dense_ref, dqkv_ref, first_ref, dfirst_ref,
):
    rows, width = x_ref.shape
    col = 256
    gain_one, shift_one = vec_ref[3:4, :], vec_ref[4:5, :]
    low = iota((1, LANES), 1) < HEAD
    keys = iota((1, SEQ_PAD), 1) < SEQ
    pairs = width // LANES

    @pl.loop(0, (rows // SEQ_PAD) * pairs)
    def _(n):
        at = tile_of(n // pairs, SEQ_PAD)
        lane = (n % pairs) * LANES
        spans = [pl.ds(pl.multiple_of(o + lane, LANES), LANES) for o in (0, width, 2 * width)]
        q, k, v = (qkv_ref[at, s] for s in spans)
        d_out = datt_ref[at, spans[0]]
        d_q, d_k, d_v = [], [], []
        for side in (low, ~low):
            q_side = jnp.where(side, q, jnp.zeros_like(q))
            scores = dot_nt(q_side, k) * head_scale
            weights = jnp.where(keys, jnp.exp(scores), 0.0)
            weights = weights * (1.0 / jnp.sum(weights, axis=-1, keepdims=True))
            d_w = dot_nt(jnp.where(side, d_out, jnp.zeros_like(d_out)), v)
            d_s = (weights * (d_w - jnp.sum(weights * d_w, axis=-1, keepdims=True)) * head_scale).astype(bf16)
            d_v.append(dot_tn(weights.astype(bf16), d_out))
            d_q.append(dot(d_s, k))
            d_k.append(dot_tn(d_s, q))
        for s, parts in zip(spans, (d_q, d_k, d_v)):
            dqkv_ref[at, s] = jnp.where(low, *parts).astype(bf16)

    @pl.loop(0, rows // ROW_TILE)
    def _(t):
        at = tile_of(t, ROW_TILE)
        normed, _ = normed_rows(x_ref[at, :])
        first_ref[at, :] = (normed * gain_one + shift_one).astype(bf16)

    @pl.loop(0, 3 * width // col)
    def _(j):
        at = tile_of(j, col)
        dense_ref[:, at] = dot_tn(first_ref[...], dqkv_ref[:, at]).astype(bf16)

    @pl.loop(0, width // col)
    def _(j):
        at = tile_of(j, col)
        wide = pl.ds(pl.multiple_of(3 * width + j * col, col), col)
        dense_ref[:, wide] = dot_tn(att_ref[...], dhb_ref[:, at]).astype(bf16)
        dfirst_ref[:, at] = dot_nt(dqkv_ref[...], w_ref[at, :])

    def step(t, sums):
        at = tile_of(t, ROW_TILE)
        d_first = dfirst_ref[at, :]
        normed, inv_std = normed_rows(x_ref[at, :])
        in_ref[at, :] = dhid_ref[at, :] + norm_row_grad(d_first * gain_one, normed, inv_std)
        add = lambda v: jnp.sum(v, axis=0, keepdims=True)
        return sums[0] + add(d_first * normed), sums[1] + add(d_first)

    zero = jnp.zeros((1, width), f32)
    gain_sum, shift_sum = lax.fori_loop(0, rows // ROW_TILE, step, (zero, zero))

    ones = jnp.ones((8, rows), bf16)
    q_sum = dot(ones, dqkv_ref[:, :width])[0:1, :]
    v_sum = dot(ones, dqkv_ref[:, 2 * width :])[0:1, :]
    order = [q_sum, v_sum, sums_ref[0:1, :], gain_sum, shift_sum, sums_ref[1:2, :], sums_ref[2:3, :]]
    stacked = jnp.concatenate(order + [jnp.zeros((LANES - len(order), width), f32)], axis=0)
    columns = jnp.transpose(stacked, (1, 0))
    router = dot_tn(sec_ref[...], dlog_ref[...])
    lane = iota((1, LANES), 1)
    columns = pltpu.roll(columns, experts, 1)
    dense_ref[:, pl.ds(4 * width, LANES)] = jnp.where(lane < experts, router, columns).astype(bf16)


def back_call(experts, x, qkv, datt, dhid, dhb, att, sec, dlog, weights, vec, sums):
    rows, width = x.shape
    shapes = (jax.ShapeDtypeStruct((rows, width), f32), jax.ShapeDtypeStruct((width, 4 * width + LANES), bf16))
    one = lambda a: pl.BlockSpec(a.shape, lambda i: (0, 0))
    return pl.pallas_call(
        functools.partial(back_kernel, experts),
        out_shape=shapes,
        grid=(1,),
        in_specs=[
            *[one(a) for a in (x, qkv, datt, dhid, dhb, att, sec, dlog)],
            pl.BlockSpec((width, 3 * width), lambda i: (0, 0)),
            one(vec),
            one(sums),
        ],
        out_specs=tuple(one(s) for s in shapes),
        scratch_shapes=[
            pltpu.VMEM((rows, 3 * width), bf16),
            pltpu.VMEM((rows, width), bf16),
            pltpu.VMEM((rows, width), f32),
        ],
        compiler_params=params(),
        cost_estimate=pl.CostEstimate(flops=15 * 10**9, bytes_accessed=35 * 10**6, transcendentals=2 * 10**6),
        name="back",
    )(x, qkv, datt, dhid, dhb, att, sec, dlog, weights, vec, sums)


def pick(value, index, axis):
    return lax.dynamic_index_in_dim(value, index, axis, keepdims=False)


def shift_along(value, axis, step):
    size = lax.axis_size("hi") * lax.axis_size("lo") if isinstance(axis, tuple) else lax.axis_size(axis)
    return lax.ppermute(value, axis, [(i, (i + step) % size) for i in range(size)])


def send_pairs(spans):
    fan, low = lax.axis_size("lo"), lax.axis_index("lo")
    got = [None] * fan
    for step in list(range(1, fan)) + [0]:
        got[step] = [shift_along(pick(s, (low + step) % fan, 0), "hi", hop) for hop, s in enumerate(spans, 1)]
    return got


def finish(mine, got):
    fan, low = lax.axis_size("lo"), lax.axis_index("lo")
    parts = [None] * fan
    for step in list(range(1, fan)) + [0]:
        value = pick(mine, (low + step) % fan, 0).astype(f32)
        for other in got[step]:
            value = value + other.astype(f32)
        if step:
            value = shift_along(value.astype(bf16), "lo", step).astype(f32)
        parts[step] = value
    return by_expert(parts)


def by_expert(parts):
    fan, low = lax.axis_size("lo"), lax.axis_index("lo")
    if fan == 1:
        return parts[0][None]
    if fan == 2:
        return jnp.stack([jnp.where(low == 0, parts[0], parts[1]), jnp.where(low == 0, parts[1], parts[0])])
    stacked = jnp.stack(parts)
    return jnp.stack([pick(stacked, (low - k) % fan, 0) for k in range(fan)])


def dense_sum(matrix):
    members = lax.axis_size("hi") * lax.axis_size("lo")
    me = lax.axis_index("hi") * lax.axis_size("lo") + lax.axis_index("lo")
    plane, spot = lax.axis_size("expert"), lax.axis_index("expert")
    rows, columns = matrix.shape
    piece = rows // (members * plane)
    current = matrix.reshape(members, plane, piece, columns)
    left, bit = plane, 1
    while left > 1:
        halves = current.reshape(members, left // 2, 2, piece, columns)
        side = (spot // bit) % 2
        sent = pick(halves, 1 - side, 2).astype(bf16)
        came = lax.ppermute(sent, "expert", [(i, i ^ bit) for i in range(plane)])
        current = pick(halves, side, 2).astype(f32) + came.astype(f32)
        left //= 2
        bit *= 2
    current = current.reshape(members, piece, columns)
    summed = pick(current, me, 0)
    for step in range(1, members):
        sent = pick(current, (me + step) % members, 0).astype(bf16)
        summed = summed + shift_along(sent, ("hi", "lo"), step).astype(f32)
    return summed


def local(
    block_in, out_grad, expert_ids, slot_ids, qkv_weight, q_bias, v_bias, out_weight, out_bias,
    norm1_gain, norm1_bias, norm2_gain, norm2_bias, router_weight, up_weight, up_bias, down_weight, down_bias,
):
    tok_rows, width = block_in.shape
    images = tok_rows // SEQ
    experts = router_weight.shape[1]
    capacity = tok_rows * 2 * 9 // (8 * experts) + 1
    slots = -(-capacity // 16) * 16
    total = experts * slots
    outer, fan, plane = lax.axis_size("hi"), lax.axis_size("lo"), lax.axis_size("expert")
    members = outer * fan
    high, low, spot = lax.axis_index("hi"), lax.axis_index("lo"), lax.axis_index("expert")
    me = high * fan + low
    hidden = up_weight.shape[2]

    def padded(values, fill=0):
        shaped = values.reshape(images, SEQ, values.shape[1])
        shaped = jnp.pad(shaped, ((0, 0), (0, SEQ_PAD - SEQ), (0, 0)), constant_values=fill)
        return shaped.reshape(images * SEQ_PAD, values.shape[1])

    def exchange(value):
        return lax.all_to_all(value, ("lo", "expert"), split_axis=0, concat_axis=0, tiled=True)

    vectors = (q_bias, v_bias, out_bias, norm1_gain, norm1_bias, norm2_gain, norm2_bias)
    extra = jnp.stack(vectors, axis=1)
    spare = jnp.zeros((extra.shape[0], LANES - experts - len(vectors)), bf16)
    packed = jnp.concatenate([qkv_weight, out_weight, router_weight, extra, spare], axis=1)
    part = packed.shape[0] // plane
    packed = lax.dynamic_slice_in_dim(packed, spot * part, part, 0)
    weights = lax.all_gather(packed, ("hi", "lo", "expert"), axis=0, tiled=True)
    small = weights[:, 4 * width :]
    vec = jnp.pad(small[:, experts : experts + len(vectors)].T.astype(f32), ((0, 1), (0, 0)))
    bias = jnp.concatenate([vec[0:1], jnp.zeros((1, width), f32), vec[1:2]], axis=1)

    up_one = pick(up_weight, low, 0)
    down_one = pick(down_weight, low, 0)
    up_shift = pick(up_bias, low, 0).astype(f32)[None]
    down_shift = pick(down_bias, low, 0).astype(f32)[None]

    owner = (expert_ids % fan) * plane + expert_ids // fan
    spots = padded(jnp.where(slot_ids >= 0, owner * slots + slot_ids, -1), -1)
    ids = padded(expert_ids, -1)
    spots_t = spots.T
    x = padded(block_in)
    cot = padded(out_grad)

    cot_sent, x = lax.optimization_barrier((place_call(spots_t, cot, total), x))
    cot_rows = exchange(cot_sent)

    qkv, att, hid, sec, probs, send = front_call(experts, total, x, weights, small, bias, vec, spots_t)
    rows_in = exchange(send)

    which = (spot * fan + low).astype(jnp.int32).reshape(1)
    grads, down_sum = gate_call(experts, which, rows_in, cot_rows, small)
    tile = 512 if (hidden // outer) % 512 == 0 else hidden // outer

    def down_span(hop, x_rows):
        part = ((high + hop) % outer).astype(jnp.int32).reshape(1)
        return down_call(x_rows, grads, up_one, up_shift, tile, part, outer).reshape(fan, hidden // members, width)

    down_away = [down_span(hop, rows_in) for hop in range(1, outer)]
    down_sent = send_pairs(down_away)
    rows_in, *_ = lax.optimization_barrier((rows_in, *down_away))
    up_grad, up_sum, outs, d_rows = expert_call(rows_in, grads, up_one, up_shift, down_one, down_shift, tile)
    up_blocks = up_grad.reshape(outer, fan, width // members, hidden)
    up_sent = send_pairs([pick(up_blocks, (high + hop) % outer, 0) for hop in range(1, outer)])
    both = jnp.concatenate([outs.reshape(-1, slots, width), d_rows.reshape(-1, slots, width)], axis=1)
    both = exchange(both)
    outs_back, rows_back = both[:, :slots].reshape(total, width), both[:, slots:].reshape(total, width)
    rows_in, _ = lax.optimization_barrier((rows_in, up_grad))
    down_mine = down_span(0, rows_in)
    down_part = finish(down_mine, down_sent)
    up_part = finish(pick(up_blocks, high, 0), up_sent)

    summary = jnp.concatenate([up_sum, down_sum], axis=1)
    small_rows = jnp.concatenate([summary] + [shift_along(summary, ("hi", "lo"), s) for s in range(1, members)], axis=0)
    from_expert = (me - jnp.arange(members)) % fan
    biases = jnp.stack(
        [jnp.sum(jnp.where((from_expert == k)[:, None], small_rows, 0.0), axis=0) for k in range(fan)]
    )
    up_shift_part = lax.dynamic_slice_in_dim(biases[:, :hidden], me * (hidden // members), hidden // members, 1)
    down_shift_part = lax.dynamic_slice_in_dim(biases[:, hidden:], me * (width // members), width // members, 1)

    block_out, d_hid, d_hid_b, d_att, d_log, sums = combine_call(
        outs_back, rows_back, cot, hid, sec, probs, spots, ids, weights, small, vec
    )
    input_grad, dense = back_call(experts, x, qkv, d_att, d_hid, d_hid_b, att, sec, d_log, weights, vec, sums)

    def unpadded(values):
        return values.reshape(images, SEQ_PAD, width)[:, :SEQ].reshape(tok_rows, width)

    dense = dense_sum(dense)
    at = 4 * width + experts
    return (
        unpadded(block_out), unpadded(input_grad),
        dense[:, : 3 * width], dense[:, at], dense[:, at + 1], dense[:, 3 * width : 4 * width],
        dense[:, at + 2], dense[:, at + 3], dense[:, at + 4], dense[:, at + 5], dense[:, at + 6],
        dense[:, 4 * width : at],
        up_part, up_shift_part, down_part, down_shift_part,
    )


def solution(mesh):
    def step(*arrays):
        members, plane = mesh.shape["dp"], mesh.shape["expert"]
        fan = arrays[14].shape[0] // plane
        split = Mesh(mesh.devices.reshape(members // fan, fan, plane), ("hi", "lo", "expert"))
        every, dp = ("hi", "lo", "expert"), ("hi", "lo")
        in_specs = (
            (P(every, None),) * 4
            + (P(dp, None), P(dp), P(dp), P(dp, None), P(dp), P(dp), P(dp), P(dp), P(dp), P(dp, None))
            + (P("expert", None, None), P("expert", None), P("expert", None, None), P("expert", None))
        )
        out_specs = (
            (P(every, None),) * 3
            + (P(every), P(every), P(every, None))
            + (P(every),) * 5
            + (P(every, None), P("expert", dp, None), P("expert", dp), P("expert", dp, None), P("expert", dp))
        )

        return jax.shard_map(local, mesh=split, in_specs=in_specs, out_specs=out_specs, check_vma=False)(*arrays)

    return step
```

```python
import functools

import jax
import jax.numpy as jnp
from jax import lax
from jax.experimental import pallas as pl
from jax.experimental.pallas import tpu as pltpu
from jax.sharding import Mesh, PartitionSpec as P


HEAD = 64
SEQ = 197

epsilon = 1e-06
inv_root_two = 0.7071067811865476
inv_root_two_pi = 0.3989422804014327

bf16 = jnp.bfloat16
f32 = jnp.float32
LANES = 128
SEQ_PAD = -(-SEQ // 16) * 16
ROW_TILE = 64
head_scale = HEAD ** (-0.5)
VMEM_MAX = 60 * 1024 * 1024


def dot(a, b):
    return jnp.dot(a, b, preferred_element_type=f32)


def dot_tn(a, b):
    return lax.dot_general(a, b, (((0,), (0,)), ((), ())), preferred_element_type=f32)


def dot_nt(a, b):
    return lax.dot_general(a, b, (((1,), (1,)), ((), ())), preferred_element_type=f32)


def iota(shape, axis):
    return lax.broadcasted_iota(jnp.int32, shape, axis)


def row_valid(start, count):
    return (iota((count, 1), 0) + start) % SEQ_PAD < SEQ


def normed_rows(values):
    centred = values - jnp.mean(values, axis=-1, keepdims=True)
    inv_std = lax.rsqrt(jnp.mean(centred * centred, axis=-1, keepdims=True) + epsilon)
    return centred * inv_std, inv_std


def norm_row_grad(scaled, normed, inv_std):
    return (
        scaled
        - jnp.mean(scaled, axis=-1, keepdims=True)
        - normed * jnp.mean(scaled * normed, axis=-1, keepdims=True)
    ) * inv_std


def tile_of(index, size):
    return pl.ds(pl.multiple_of(index * size, size), size)


def pad_rows(source_ref, padded_ref):
    width = source_ref.shape[1]
    for i in range(source_ref.shape[0] // SEQ):
        padded_ref[i * SEQ_PAD : i * SEQ_PAD + SEQ, :] = source_ref[i * SEQ : (i + 1) * SEQ, :]
        padded_ref[i * SEQ_PAD + SEQ : (i + 1) * SEQ_PAD, :] = jnp.zeros((SEQ_PAD - SEQ, width), f32)


def unpad_rows(padded_ref, out_ref):
    for i in range(out_ref.shape[0] // SEQ):
        out_ref[i * SEQ : (i + 1) * SEQ, :] = padded_ref[i * SEQ_PAD : i * SEQ_PAD + SEQ, :]


def front_kernel(
    experts, source_ref, w_ref, small_ref, spots_ref,
    qkv_ref, att_ref, hid_ref, sec_ref, probs_ref, send_ref, vec_ref, x_ref, first_ref, bias_ref,
):
    rows, width = x_ref.shape
    col = 256
    pad_rows(source_ref, x_ref)
    turned = jnp.transpose(small_ref[...].astype(f32), (1, 0))
    vec_ref[...] = pltpu.roll(turned, LANES - experts, 0)[0:8, :]
    bias_ref[:, :width] = vec_ref[0:1, :]
    bias_ref[:, width : 2 * width] = jnp.zeros((1, width), f32)
    bias_ref[:, 2 * width :] = vec_ref[1:2, :]
    gain_one, shift_one = vec_ref[3:4, :], vec_ref[4:5, :]
    gain_two, shift_two = vec_ref[5:6, :], vec_ref[6:7, :]

    @pl.loop(0, rows // ROW_TILE)
    def _(t):
        at = tile_of(t, ROW_TILE)
        normed, _ = normed_rows(x_ref[at, :])
        first_ref[at, :] = (normed * gain_one + shift_one).astype(bf16)

    valid = row_valid(0, rows)

    @pl.loop(0, 3 * width // col)
    def _(j):
        at = tile_of(j, col)
        got = dot(first_ref[...], w_ref[:, at]) + bias_ref[:, at]
        got = got * jnp.where(j < width // col, head_scale, 1.0)
        qkv_ref[:, at] = jnp.where(valid, got, 0.0).astype(bf16)

    low = iota((1, LANES), 1) < HEAD
    keys = jnp.where(iota((SEQ_PAD, 1), 0) < SEQ, 1.0, 0.0).astype(bf16)
    ones_low = jnp.where(low, keys, jnp.zeros_like(keys))
    ones_high = jnp.where(low, jnp.zeros_like(keys), keys)
    pairs = width // LANES

    @pl.loop(0, (rows // SEQ_PAD) * pairs)
    def _(n):
        at = tile_of(n // pairs, SEQ_PAD)
        lane = (n % pairs) * LANES
        q = qkv_ref[at, pl.ds(pl.multiple_of(lane, LANES), LANES)]
        k = qkv_ref[at, pl.ds(pl.multiple_of(width + lane, LANES), LANES)]
        v = qkv_ref[at, pl.ds(pl.multiple_of(2 * width + lane, LANES), LANES)]
        zero = jnp.zeros_like(q)
        grown = jnp.exp(dot_nt(jnp.where(low, q, zero), k)).astype(bf16)
        first = dot(grown, jnp.where(low, v, ones_high))
        grown = jnp.exp(dot_nt(jnp.where(low, zero, q), k)).astype(bf16)
        second = dot(grown, jnp.where(low, ones_low, v))
        sums = pltpu.roll(jnp.where(low, second, first), HEAD, 1)
        att_ref[at, pl.ds(pl.multiple_of(lane, LANES), LANES)] = (jnp.where(low, first, second) / sums).astype(bf16)

    @pl.loop(0, width // col)
    def _(j):
        at = tile_of(j, col)
        wide = pl.ds(pl.multiple_of(3 * width + j * col, col), col)
        hid_ref[:, at] = x_ref[:, at] + dot(att_ref[...], w_ref[:, wide]) + vec_ref[2:3, at]

    lanes = iota((1, LANES), 1) < experts

    @pl.loop(0, rows // ROW_TILE)
    def _(t):
        at = tile_of(t, ROW_TILE)
        normed, _ = normed_rows(hid_ref[at, :])
        ok = row_valid(t * ROW_TILE, ROW_TILE)
        second = jnp.where(ok, normed * gain_two + shift_two, 0.0).astype(bf16)
        sec_ref[at, :] = second
        grown = jnp.where(lanes, jnp.exp(jnp.where(lanes, dot(second, small_ref[...]), 0.0)), 0.0)
        probs_ref[at, :] = grown / jnp.sum(grown, axis=-1, keepdims=True)

    place_rows(spots_ref, sec_ref, send_ref)


def place_rows(spots_ref, rows_ref, send_ref):
    total, rows = send_ref.shape[0], rows_ref.shape[0]
    block = total // 4

    @pl.loop(0, 4)
    def _(d):
        labels = iota((block, rows), 0) + d * block
        hit = (labels == spots_ref[0:1, :]) | (labels == spots_ref[1:2, :])
        send_ref[tile_of(d, block), :] = dot(jnp.where(hit, 1.0, 0.0).astype(bf16), rows_ref[...]).astype(bf16)


def flipped(index, mask):
    return index + mask - 2 * mask * ((index // mask) % 2)


def gather_kernel(
    outer, fan, qkv_ref, out_ref, small_ref, cot_ref, spots_ref,
    w_ref, all_small_ref, send_ref, held_ref, held_small_ref, cot_pad_ref, cot_low_ref, send_sem, recv_sem, local_sem,
):
    members = outer * fan
    high, low, spot = lax.axis_index("hi"), lax.axis_index("lo"), lax.axis_index("expert")
    me = high * fan + low
    rows, cols = held_ref.shape
    mine = spot % 8
    in_qkv = qkv_ref.shape[1] // cols
    mesh_id = pl.DeviceIdType.MESH

    def member(step):
        to = (me + step) % members
        return (to // fan, to % fan, spot)

    def near(mask):
        return (high, low, flipped(spot, mask))

    barrier = pltpu.get_barrier_semaphore()
    peers = [member(s) for s in range(1, members)] + [near(b) for b in (4, 2, 1)]
    for peer in peers:
        pl.semaphore_signal(barrier, inc=1, device_id=peer, device_id_type=mesh_id)

    @pl.when(mine < in_qkv)
    def _():
        span = pl.ds(pl.multiple_of(mine * cols, cols), cols)
        copy = pltpu.make_async_copy(qkv_ref.at[:, span], held_ref, local_sem.at[0])
        copy.start()
        copy.wait()

    @pl.when(mine >= in_qkv)
    def _():
        span = pl.ds(pl.multiple_of((mine - in_qkv) * cols, cols), cols)
        copy = pltpu.make_async_copy(out_ref.at[:, span], held_ref, local_sem.at[0])
        copy.start()
        copy.wait()

    copy = pltpu.make_async_copy(small_ref, held_small_ref, local_sem.at[1])
    copy.start()
    copy.wait()
    pl.semaphore_wait(barrier, len(peers))

    def block(step, masks):
        source = (me - step + members) % members
        span = mine
        for mask in masks:
            span = flipped(span, mask)
        return w_ref.at[
            pl.ds(pl.multiple_of(source * rows, rows), rows), pl.ds(pl.multiple_of(span * cols, cols), cols)
        ]

    copies = []

    def send(source, target, device):
        k = len(copies)
        copies.append(
            pltpu.make_async_remote_copy(
                src_ref=source, dst_ref=target, send_sem=send_sem.at[k], recv_sem=recv_sem.at[k],
                device_id=device, device_id_type=mesh_id,
            )
        )
        copies[-1].start()
        return copies[-1]

    stay = [
        pltpu.make_async_copy(held_ref, block(0, ()), local_sem.at[0]),
        pltpu.make_async_copy(
            held_small_ref, all_small_ref.at[pl.ds(pl.multiple_of(me * rows, rows), rows), :], local_sem.at[1]
        ),
    ]
    own = all_small_ref.at[pl.ds(pl.multiple_of(me * rows, rows), rows), :]
    over = [None] + [send(held_ref, block(0, ()), member(s)) for s in range(1, members)]
    near_by = [{b: send(held_ref, block(0, ()), near(b)) for b in (4, 2, 1)}]
    late = [send(held_small_ref, own, member(s)) for s in range(1, members)]
    for copy in stay:
        copy.start()
    for s in range(1, members):
        over[s].wait_recv()
        near_by.append({b: send(block(s, ()), block(s, ()), near(b)) for b in (4, 2, 1)})

    pad_rows(cot_ref, cot_pad_ref)
    cot_low_ref[...] = cot_pad_ref[...].astype(bf16)
    place_rows(spots_ref, cot_low_ref, send_ref)

    relays = []
    for s in range(members):
        first, second = (4, 2) if s % 2 == 0 else (2, 4)
        near_by[s][first].wait_recv()
        relays.append(send(block(s, (first,)), block(s, (first,)), near(second)))
        late.append(send(block(s, (first,)), block(s, (first,)), near(1)))
        near_by[s][second].wait_recv()
        late.append(send(block(s, (second,)), block(s, (second,)), near(1)))
    for s in range(members):
        relays[s].wait_recv()
        late.append(send(block(s, (4, 2)), block(s, (4, 2)), near(1)))
    for s in range(members):
        near_by[s][1].wait_recv()
    for copy in late:
        copy.wait_recv()
    for copy in copies:
        copy.wait_send()
    for copy in stay:
        copy.wait()


def gather_call(outer, fan, total, qkv, out, small, cot, spots):
    rows, width = out.shape
    members = outer * fan
    cols = 4 * width // 8
    count = 2 * (members - 1) + 3 * members + 4 * members
    anywhere = pl.BlockSpec(memory_space=pl.ANY)
    padded = cot.shape[0] // SEQ * SEQ_PAD
    return pl.pallas_call(
        functools.partial(gather_kernel, outer, fan),
        out_shape=(
            jax.ShapeDtypeStruct((members * rows, 4 * width), bf16),
            jax.ShapeDtypeStruct((members * rows, LANES), bf16),
            jax.ShapeDtypeStruct((total, width), bf16),
        ),
        in_specs=[anywhere] * 3 + whole(2),
        out_specs=(anywhere, anywhere, whole(1)[0]),
        scratch_shapes=[
            pltpu.VMEM((rows, cols), bf16),
            pltpu.VMEM((rows, LANES), bf16),
            pltpu.VMEM((padded, width), f32),
            pltpu.VMEM((padded, width), bf16),
            pltpu.SemaphoreType.DMA((count,)),
            pltpu.SemaphoreType.DMA((count,)),
            pltpu.SemaphoreType.DMA((2,)),
        ],
        compiler_params=params(collective_id=0, has_side_effects=True),
        cost_estimate=pl.CostEstimate(flops=25 * 10**8, bytes_accessed=40 * 10**6, transcendentals=0),
        name="gather",
    )(qkv, out, small, cot, spots)


def whole(n):
    return [pl.BlockSpec(memory_space=pltpu.VMEM)] * n


def params(**more):
    return pltpu.CompilerParams(vmem_limit_bytes=VMEM_MAX, **more)


def front_call(experts, total, x, weights, small, spots):
    width = x.shape[1]
    rows = x.shape[0] // SEQ * SEQ_PAD
    shapes = (
        jax.ShapeDtypeStruct((rows, 3 * width), bf16),
        jax.ShapeDtypeStruct((rows, width), bf16),
        jax.ShapeDtypeStruct((rows, width), f32),
        jax.ShapeDtypeStruct((rows, width), bf16),
        jax.ShapeDtypeStruct((rows, LANES), f32),
        jax.ShapeDtypeStruct((total, width), bf16),
        jax.ShapeDtypeStruct((8, width), f32),
    )
    return pl.pallas_call(
        functools.partial(front_kernel, experts),
        out_shape=shapes,
        in_specs=whole(4),
        out_specs=tuple(whole(7)),
        scratch_shapes=[
            pltpu.VMEM((rows, width), f32),
            pltpu.VMEM((rows, width), bf16),
            pltpu.VMEM((1, 3 * width), f32),
        ],
        compiler_params=params(),
        cost_estimate=pl.CostEstimate(flops=14 * 10**9, bytes_accessed=30 * 10**6, transcendentals=2 * 10**6),
        name="front",
    )(x, weights, small, spots)


def gelu_parts(pre_act):
    cumulative = 0.5 * (1.0 + lax.erf(pre_act * inv_root_two))
    return pre_act * cumulative, cumulative


def gate_kernel(experts, which_ref, x_ref, cot_ref, small_ref, grad_ref, sum_ref):
    lane = iota((1, LANES), 1)
    mine = lane == which_ref[0]
    total = jnp.zeros((1, cot_ref.shape[1]), f32)
    rows = x_ref.shape[0]
    size = rows // 4

    def step(t, total):
        at = tile_of(t, size)
        logits = jnp.where(lane < experts, dot(x_ref[at, :], small_ref[...]), 0.0)
        grown = jnp.where(lane < experts, jnp.exp(logits), 0.0)
        gate = jnp.sum(jnp.where(mine, grown, 0.0), axis=-1, keepdims=True) / jnp.sum(grown, axis=-1, keepdims=True)
        scaled = (gate * cot_ref[at, :].astype(f32)).astype(bf16)
        grad_ref[at, :] = scaled
        return total + jnp.sum(scaled.astype(f32), axis=0, keepdims=True)

    sum_ref[...] = lax.fori_loop(0, rows // size, step, total)


def gate_call(experts, which, rows_in, cot, small):
    return pl.pallas_call(
        functools.partial(gate_kernel, experts),
        out_shape=(jax.ShapeDtypeStruct(cot.shape, bf16), jax.ShapeDtypeStruct((1, cot.shape[1]), f32)),
        in_specs=[pl.BlockSpec(memory_space=pltpu.SMEM)] + whole(3),
        out_specs=tuple(whole(2)),
        compiler_params=params(),
        cost_estimate=pl.CostEstimate(flops=10**9, bytes_accessed=3 * cot.size * 2, transcendentals=10**5),
        name="gate",
    )(which, rows_in, cot, small)


def down_kernel(steps, x_ref, grad_ref, up_ref, shift_ref, *refs):
    *out_refs, act_ref = refs
    rows = x_ref.shape[0]
    size = rows // 4

    @pl.loop(0, 4)
    def _(t):
        at = tile_of(t, size)
        act_ref[at, :] = gelu_parts(dot(x_ref[at, :], up_ref[...]) + shift_ref[...])[0].astype(bf16)

    got = dot_tn(act_ref[...], grad_ref[...]).astype(bf16)
    for i, out_ref in enumerate(out_refs):

        @pl.when(pl.program_id(0) // steps == i)
        def _(out_ref=out_ref):
            out_ref[...] = got


def down_call(x, grads, up, shift, where, members):
    rows, width = x.shape
    span = up.shape[1] // members
    tile = 384 if span % 384 == 0 else span
    steps = span // tile
    count = where.shape[0]
    grid = pltpu.PrefetchScalarGridSpec(
        num_scalar_prefetch=1,
        grid=(count * steps,),
        in_specs=[
            pl.BlockSpec((rows, width), lambda j, p: (0, 0)),
            pl.BlockSpec((rows, width), lambda j, p: (0, 0)),
            pl.BlockSpec((width, tile), lambda j, p: (0, p[j // steps] * steps + j % steps)),
            pl.BlockSpec((1, tile), lambda j, p: (0, p[j // steps] * steps + j % steps)),
        ],
        out_specs=[
            pl.BlockSpec((tile, width), lambda j, p, i=i: (jnp.clip(j - i * steps, 0, steps - 1), 0))
            for i in range(count)
        ],
        scratch_shapes=[pltpu.VMEM((rows, tile), bf16)],
    )
    return pl.pallas_call(
        lambda p_ref, *refs: down_kernel(steps, *refs),
        out_shape=[jax.ShapeDtypeStruct((span, width), bf16)] * count,
        grid_spec=grid,
        compiler_params=params(dimension_semantics=("arbitrary",)),
        cost_estimate=pl.CostEstimate(flops=4 * rows * width * span * count, bytes_accessed=4 * rows * width + 4 * span * width * count, transcendentals=rows * span),
        name="down",
    )(where, x, grads, up, shift)


def expert_kernel(where_ref, x_ref, grad_ref, up_ref, shift_ref, down_ref, down_shift_ref, *refs):
    *upg_refs, upsum_ref, both_ref, dpre_ref, upg_ref, out_acc, rows_acc = refs
    j = pl.program_id(0)
    rows, width = x_ref.shape
    tile = up_ref.shape[1]
    size = rows // 4
    span = width // len(upg_refs)

    @pl.when(j == 0)
    def _():
        out_acc[...] = jnp.broadcast_to(down_shift_ref[...], out_acc.shape)
        rows_acc[...] = jnp.zeros_like(rows_acc)

    def step(t, total):
        at = tile_of(t, size)
        pre = dot(x_ref[at, :], up_ref[...]) + shift_ref[...]
        act, cumulative = gelu_parts(pre)
        slope = cumulative + pre * jnp.exp(-0.5 * pre * pre) * inv_root_two_pi
        d_pre = dot_nt(grad_ref[at, :], down_ref[...]) * slope
        d_pre_b = d_pre.astype(bf16)
        dpre_ref[at, :] = d_pre_b
        out_acc[at, :] += dot(act.astype(bf16), down_ref[...])
        rows_acc[at, :] += dot_nt(d_pre_b, up_ref[...])
        return total + jnp.sum(d_pre, axis=0, keepdims=True)

    upsum_ref[...] = lax.fori_loop(0, 4, step, jnp.zeros((1, tile), f32))
    upg_ref[...] = dot_tn(x_ref[...], dpre_ref[...]).astype(bf16)
    for i, ref in enumerate(upg_refs):
        ref[...] = upg_ref[pl.ds(pl.multiple_of(where_ref[i] * span, span), span), :]

    @pl.when(j == pl.num_programs(0) - 1)
    def _():
        experts, _, slots, _ = both_ref.shape

        @pl.loop(0, experts)
        def _(e):
            at = tile_of(e, slots)
            both_ref[e, 0] = out_acc[at, :].astype(bf16)
            both_ref[e, 1] = rows_acc[at, :].astype(bf16)


def expert_call(x, grads, up, shift, down, down_shift, where, experts, tile):
    rows, width = x.shape
    hidden = up.shape[1]
    count = where.shape[0]
    fixed = lambda *shape: pl.BlockSpec(shape, lambda j, p: (0,) * len(shape))
    both = (experts, 2, rows // experts, width)
    grid = pltpu.PrefetchScalarGridSpec(
        num_scalar_prefetch=1,
        grid=(hidden // tile,),
        in_specs=[
            fixed(rows, width),
            fixed(rows, width),
            pl.BlockSpec((width, tile), lambda j, p: (0, j)),
            pl.BlockSpec((1, tile), lambda j, p: (0, j)),
            pl.BlockSpec((tile, width), lambda j, p: (j, 0)),
            fixed(1, width),
        ],
        out_specs=[pl.BlockSpec((width // count, tile), lambda j, p: (0, j))] * count
        + [pl.BlockSpec((1, tile), lambda j, p: (0, j)), fixed(*both)],
        scratch_shapes=[
            pltpu.VMEM((rows, tile), bf16),
            pltpu.VMEM((width, tile), bf16),
            pltpu.VMEM((rows, width), f32),
            pltpu.VMEM((rows, width), f32),
        ],
    )
    got = pl.pallas_call(
        expert_kernel,
        out_shape=[jax.ShapeDtypeStruct((width // count, hidden), bf16)] * count
        + [jax.ShapeDtypeStruct((1, hidden), f32), jax.ShapeDtypeStruct(both, bf16)],
        grid_spec=grid,
        compiler_params=params(dimension_semantics=("arbitrary",)),
        cost_estimate=pl.CostEstimate(flops=10 * rows * width * hidden, bytes_accessed=8 * rows * width + 6 * hidden * width, transcendentals=2 * rows * hidden),
        name="expert",
    )(where, x, grads, up, shift, down, down_shift)
    return got[:count], got[count], got[count + 1]


def combine_kernel(
    both_ref, source_ref, hid_ref, probs_ref, spots_ref, ids_ref, w_ref, small_ref, vec_ref,
    block_ref, dhid_ref, dhb_ref, datt_ref, dlog_ref, sums_ref, outs_ref, back_ref, cot_ref, blk_ref,
):
    rows, width = cot_ref.shape
    total = outs_ref.shape[0]
    experts, _, slots, _ = both_ref.shape
    pad_rows(source_ref, cot_ref)

    @pl.loop(0, experts)
    def _(e):
        at = tile_of(e, slots)
        outs_ref[at, :] = both_ref[e, 0]
        back_ref[at, :] = both_ref[e, 1]

    size = SEQ_PAD
    gain_two = vec_ref[5:6, :]
    labels = iota((1, total), 1)
    lane = iota((1, LANES), 1)

    def step(t, sums):
        at = tile_of(t, size)
        first = jnp.where(spots_ref[at, 0:1] == labels, 1.0, 0.0).astype(bf16)
        second = jnp.where(spots_ref[at, 1:2] == labels, 1.0, 0.0).astype(bf16)
        got0, got1 = dot(first, outs_ref[...]), dot(second, outs_ref[...])
        back = dot(first + second, back_ref[...])
        probs = probs_ref[at, :]
        hot0 = jnp.where(ids_ref[at, 0:1] == lane, 1.0, 0.0)
        hot1 = jnp.where(ids_ref[at, 1:2] == lane, 1.0, 0.0)
        gate0 = jnp.sum(probs * hot0, axis=-1, keepdims=True)
        gate1 = jnp.sum(probs * hot1, axis=-1, keepdims=True)
        cot = cot_ref[at, :]
        hid = hid_ref[at, :]
        blk_ref[at, :] = hid + gate0 * got0 + gate1 * got1
        d0 = jnp.sum(cot * got0, axis=-1, keepdims=True)
        d1 = jnp.sum(cot * got1, axis=-1, keepdims=True)
        d_probs = d0 * hot0 + d1 * hot1
        d_logits = (probs * (d_probs - jnp.sum(probs * d_probs, axis=-1, keepdims=True))).astype(bf16)
        dlog_ref[at, :] = d_logits
        d_second = dot_nt(d_logits, small_ref[...]) + back
        normed, inv_std = normed_rows(hid)
        d_hidden = cot + norm_row_grad(d_second * gain_two, normed, inv_std)
        dhid_ref[at, :] = d_hidden
        d_hidden_b = d_hidden.astype(bf16)
        dhb_ref[at, :] = d_hidden_b
        datt_ref[at, :] = dot_nt(d_hidden_b, w_ref[...]).astype(bf16)
        add = lambda v: jnp.sum(v, axis=0, keepdims=True)
        return tuple(s + add(v) for s, v in zip(sums, (d_hidden, d_second * normed, d_second)))

    zero = jnp.zeros((1, width), f32)
    sums = lax.fori_loop(0, rows // size, step, (zero, zero, zero))
    for i, s in enumerate(sums):
        sums_ref[i : i + 1, :] = s
    unpad_rows(blk_ref, block_ref)


def combine_call(both, cot, hid, probs, spots, ids, weights, small, vec):
    rows, width = hid.shape
    total = both.shape[0] * both.shape[2]
    shapes = (
        jax.ShapeDtypeStruct(cot.shape, f32),
        jax.ShapeDtypeStruct((rows, width), f32),
        jax.ShapeDtypeStruct((rows, width), bf16),
        jax.ShapeDtypeStruct((rows, width), bf16),
        jax.ShapeDtypeStruct((rows, LANES), bf16),
        jax.ShapeDtypeStruct((8, width), f32),
    )
    full = lambda a: pl.BlockSpec(a.shape, lambda i: (0,) * len(a.shape))
    return pl.pallas_call(
        combine_kernel,
        out_shape=shapes,
        grid=(1,),
        in_specs=[
            *[full(a) for a in (both, cot, hid, probs, spots, ids)],
            pl.BlockSpec((width, width), lambda i: (0, 3)),
            full(small),
            full(vec),
        ],
        out_specs=tuple(full(a) for a in shapes),
        scratch_shapes=[
            pltpu.VMEM((total, width), bf16),
            pltpu.VMEM((total, width), bf16),
            pltpu.VMEM((rows, width), f32),
            pltpu.VMEM((rows, width), f32),
        ],
        compiler_params=params(),
        cost_estimate=pl.CostEstimate(flops=8 * 10**9, bytes_accessed=25 * 10**6, transcendentals=0),
        name="combine",
    )(both, cot, hid, probs, spots, ids, weights, small, vec)


def back_kernel(
    experts, source_ref, qkv_ref, datt_ref, dhid_ref, dhb_ref, att_ref, sec_ref, dlog_ref, w_ref, vec_ref, sums_ref,
    input_ref, dense_ref, dqkv_ref, first_ref, dfirst_ref, x_ref,
):
    rows, width = x_ref.shape
    pad_rows(source_ref, x_ref)
    col = 256
    gain_one, shift_one = vec_ref[3:4, :], vec_ref[4:5, :]
    low = iota((1, LANES), 1) < HEAD
    keys = iota((SEQ_PAD, 1), 0) < SEQ
    lower = iota((LANES, 1), 0) < HEAD
    pairs = width // LANES

    @pl.loop(0, (rows // SEQ_PAD) * pairs)
    def _(n):
        at = tile_of(n // pairs, SEQ_PAD)
        lane = (n % pairs) * LANES
        spans = [pl.ds(pl.multiple_of(o + lane, LANES), LANES) for o in (0, width, 2 * width)]
        q, k, v = (qkv_ref[at, s] for s in spans)
        d_out = datt_ref[at, spans[0]]
        k_turned = jnp.transpose(k, (1, 0))
        zero = jnp.zeros_like(q)
        d_q, d_k, d_v = [], [], []
        for side in (low, ~low):
            grown = jnp.where(keys, jnp.exp(dot_nt(k, jnp.where(side, q, zero))), 0.0)
            weights = grown * (1.0 / jnp.sum(grown, axis=0, keepdims=True))
            d_w = dot_nt(v, jnp.where(side, d_out, zero))
            d_s = (weights * (d_w - jnp.sum(weights * d_w, axis=0, keepdims=True))).astype(bf16)
            d_v.append(dot(weights.astype(bf16), d_out))
            d_k.append(dot(d_s, q))
            d_q.append(dot(k_turned, d_s))
        d_query = jnp.transpose(jnp.where(lower, *d_q) * head_scale, (1, 0))
        dqkv_ref[at, spans[0]] = d_query.astype(bf16)
        dqkv_ref[at, spans[1]] = jnp.where(low, *d_k).astype(bf16)
        dqkv_ref[at, spans[2]] = jnp.where(low, *d_v).astype(bf16)

    @pl.loop(0, rows // ROW_TILE)
    def _(t):
        at = tile_of(t, ROW_TILE)
        normed, _ = normed_rows(x_ref[at, :])
        first_ref[at, :] = (normed * gain_one + shift_one).astype(bf16)

    @pl.loop(0, 3 * width // col)
    def _(j):
        at = tile_of(j, col)
        dense_ref[:, at] = dot_tn(first_ref[...], dqkv_ref[:, at]).astype(bf16)

    @pl.loop(0, width // col)
    def _(j):
        at = tile_of(j, col)
        wide = pl.ds(pl.multiple_of(3 * width + j * col, col), col)
        dense_ref[:, wide] = dot_tn(att_ref[...], dhb_ref[:, at]).astype(bf16)
        dfirst_ref[:, at] = dot_nt(dqkv_ref[...], w_ref[at, :])

    def step(t, sums):
        at = tile_of(t, ROW_TILE)
        d_first = dfirst_ref[at, :]
        normed, inv_std = normed_rows(x_ref[at, :])
        dfirst_ref[at, :] = dhid_ref[at, :] + norm_row_grad(d_first * gain_one, normed, inv_std)
        add = lambda v: jnp.sum(v, axis=0, keepdims=True)
        return sums[0] + add(d_first * normed), sums[1] + add(d_first)

    zero = jnp.zeros((1, width), f32)
    gain_sum, shift_sum = lax.fori_loop(0, rows // ROW_TILE, step, (zero, zero))
    unpad_rows(dfirst_ref, input_ref)

    ones = jnp.ones((8, rows), bf16)
    q_sum = dot(ones, dqkv_ref[:, :width])[0:1, :]
    v_sum = dot(ones, dqkv_ref[:, 2 * width :])[0:1, :]
    order = [q_sum, v_sum, sums_ref[0:1, :], gain_sum, shift_sum, sums_ref[1:2, :], sums_ref[2:3, :]]
    stacked = jnp.concatenate(order + [jnp.zeros((LANES - len(order), width), f32)], axis=0)
    columns = jnp.transpose(stacked, (1, 0))
    router = dot_tn(sec_ref[...], dlog_ref[...])
    lane = iota((1, LANES), 1)
    columns = pltpu.roll(columns, experts, 1)
    dense_ref[:, pl.ds(4 * width, LANES)] = jnp.where(lane < experts, router, columns).astype(bf16)


def back_call(experts, x, qkv, datt, dhid, dhb, att, sec, dlog, weights, vec, sums):
    rows, width = dhid.shape
    shapes = (jax.ShapeDtypeStruct(x.shape, f32), jax.ShapeDtypeStruct((width, 4 * width + LANES), bf16))
    one = lambda a: pl.BlockSpec(a.shape, lambda i: (0, 0))
    return pl.pallas_call(
        functools.partial(back_kernel, experts),
        out_shape=shapes,
        grid=(1,),
        in_specs=[
            *[one(a) for a in (x, qkv, datt, dhid, dhb, att, sec, dlog)],
            pl.BlockSpec((width, 3 * width), lambda i: (0, 0)),
            one(vec),
            one(sums),
        ],
        out_specs=tuple(one(s) for s in shapes),
        scratch_shapes=[
            pltpu.VMEM((rows, 3 * width), bf16),
            pltpu.VMEM((rows, width), bf16),
            pltpu.VMEM((rows, width), f32),
            pltpu.VMEM((rows, width), f32),
        ],
        compiler_params=params(),
        cost_estimate=pl.CostEstimate(flops=15 * 10**9, bytes_accessed=35 * 10**6, transcendentals=2 * 10**6),
        name="back",
    )(x, qkv, datt, dhid, dhb, att, sec, dlog, weights, vec, sums)


def pick(value, index, axis):
    return lax.dynamic_index_in_dim(value, index, axis, keepdims=False)


def shift_along(value, axis, step):
    size = lax.axis_size("hi") * lax.axis_size("lo") if isinstance(axis, tuple) else lax.axis_size(axis)
    return lax.ppermute(value, axis, [(i, (i + step) % size) for i in range(size)])


def send_pairs(spans):
    got = []
    for step in range(lax.axis_size("lo")):
        got.append([shift_along(s[step], "hi", hop) for hop, s in enumerate(spans, 1)])
    return got


def finish(mine, got):
    fan = lax.axis_size("lo")
    parts = [None] * fan
    for step in list(range(1, fan)) + [0]:
        value = mine[step].astype(f32)
        for other in got[step]:
            value = value + other.astype(f32)
        if step:
            value = shift_along(value.astype(bf16), "lo", step).astype(f32)
        parts[step] = value
    return by_expert(parts)


def by_expert(parts):
    fan, low = lax.axis_size("lo"), lax.axis_index("lo")
    if fan == 1:
        return parts[0][None]
    if fan == 2:
        return jnp.stack([jnp.where(low == 0, parts[0], parts[1]), jnp.where(low == 0, parts[1], parts[0])])
    stacked = jnp.stack(parts)
    return jnp.stack([pick(stacked, (low - k) % fan, 0) for k in range(fan)])


def dense_sum(matrix):
    members = lax.axis_size("hi") * lax.axis_size("lo")
    me = lax.axis_index("hi") * lax.axis_size("lo") + lax.axis_index("lo")
    plane, spot = lax.axis_size("expert"), lax.axis_index("expert")
    rows, columns = matrix.shape
    piece = rows // (members * plane)
    current = matrix.reshape(members, plane, piece, columns)
    left, bit = plane, 1
    while left > 1:
        halves = current.reshape(members, left // 2, 2, piece, columns)
        side = (spot // bit) % 2
        sent = pick(halves, 1 - side, 2).astype(bf16)
        came = lax.ppermute(sent, "expert", [(i, i ^ bit) for i in range(plane)])
        current = pick(halves, side, 2).astype(f32) + came.astype(f32)
        left //= 2
        bit *= 2
    current = current.reshape(members, piece, columns)
    summed = pick(current, me, 0)
    for step in range(1, members):
        sent = pick(current, (me + step) % members, 0).astype(bf16)
        summed = summed + shift_along(sent, ("hi", "lo"), step).astype(f32)
    return summed


def local(
    block_in, out_grad, expert_ids, slot_ids, qkv_weight, q_bias, v_bias, out_weight, out_bias,
    norm1_gain, norm1_bias, norm2_gain, norm2_bias, router_weight, up_weight, up_bias, down_weight, down_bias,
):
    tok_rows, width = block_in.shape
    images = tok_rows // SEQ
    experts = router_weight.shape[1]
    capacity = tok_rows * 2 * 9 // (8 * experts) + 1
    slots = -(-capacity // 16) * 16
    total = experts * slots
    outer, fan, plane = lax.axis_size("hi"), lax.axis_size("lo"), lax.axis_size("expert")
    members = outer * fan
    high, low, spot = lax.axis_index("hi"), lax.axis_index("lo"), lax.axis_index("expert")
    me = high * fan + low
    hidden = up_weight.shape[2]

    def padded(values):
        shaped = values.reshape(images, SEQ, values.shape[1])
        shaped = jnp.pad(shaped, ((0, 0), (0, SEQ_PAD - SEQ), (0, 0)), constant_values=-1)
        return shaped.reshape(images * SEQ_PAD, values.shape[1])

    def exchange(value):
        return lax.all_to_all(value, ("lo", "expert"), split_axis=0, concat_axis=0, tiled=True)

    vectors = (q_bias, v_bias, out_bias, norm1_gain, norm1_bias, norm2_gain, norm2_bias)
    extra = jnp.stack(vectors, axis=1)
    spare = jnp.zeros((extra.shape[0], LANES - experts - len(vectors)), bf16)
    extra = jnp.concatenate([router_weight, extra, spare], axis=1)
    owner = (expert_ids % fan) * plane + expert_ids // fan
    spots = padded(jnp.where(slot_ids >= 0, owner * slots + slot_ids, -1))
    ids = padded(expert_ids)
    spots_t = spots.T

    weights, small, cot_sent = gather_call(outer, fan, total, qkv_weight, out_weight, extra, out_grad, spots_t)
    cot_rows = exchange(cot_sent)
    qkv, att, hid, sec, probs, send, vec = front_call(experts, total, block_in, weights, small, spots_t)
    rows_in = exchange(send)

    up_one = pick(up_weight, low, 0)
    down_one = pick(down_weight, low, 0)
    up_shift = pick(up_bias, low, 0).astype(f32)[None]
    down_shift = pick(down_bias, low, 0).astype(f32)[None]

    which = (spot * fan + low).astype(jnp.int32).reshape(1)
    grads, down_sum = gate_call(experts, which, rows_in, cot_rows, small)
    tile = 512 if (hidden // outer) % 512 == 0 else hidden // outer
    names = [[(high + hop) % outer * fan + (low + step) % fan for step in range(fan)] for hop in range(outer)]

    def down_span(hop, x_rows):
        order = list(range(1, fan)) + [0]
        got = down_call(x_rows, grads, up_one, up_shift, jnp.stack([names[hop][s] for s in order]), members)
        return [got[order.index(s)] for s in range(fan)]

    down_away = [down_span(hop, rows_in) for hop in range(1, outer)]
    down_sent = send_pairs(down_away)
    rows_in, *_ = lax.optimization_barrier((rows_in, *down_away))
    flat = jnp.stack([m for row in names for m in row])
    ups, up_sum, both = expert_call(
        rows_in, grads, up_one, up_shift, down_one, down_shift, flat, experts, tile
    )
    ups = [ups[hop * fan : (hop + 1) * fan] for hop in range(outer)]
    up_sent = send_pairs(ups[1:])
    both = exchange(both)
    rows_in, _ = lax.optimization_barrier((rows_in, up_sum))
    down_mine = down_span(0, rows_in)
    down_part = finish(down_mine, down_sent)
    up_part = finish(ups[0], up_sent)

    summary = jnp.concatenate([up_sum, down_sum], axis=1)
    small_rows = jnp.concatenate([summary] + [shift_along(summary, ("hi", "lo"), s) for s in range(1, members)], axis=0)
    from_expert = (me - jnp.arange(members)) % fan
    biases = jnp.stack(
        [jnp.sum(jnp.where((from_expert == k)[:, None], small_rows, 0.0), axis=0) for k in range(fan)]
    )
    up_shift_part = lax.dynamic_slice_in_dim(biases[:, :hidden], me * (hidden // members), hidden // members, 1)
    down_shift_part = lax.dynamic_slice_in_dim(biases[:, hidden:], me * (width // members), width // members, 1)

    block_out, d_hid, d_hid_b, d_att, d_log, sums = combine_call(
        both, out_grad, hid, probs, spots, ids, weights, small, vec
    )
    input_grad, dense = back_call(experts, block_in, qkv, d_att, d_hid, d_hid_b, att, sec, d_log, weights, vec, sums)

    dense = dense_sum(dense)
    at = 4 * width + experts
    return (
        block_out, input_grad,
        dense[:, : 3 * width], dense[:, at], dense[:, at + 1], dense[:, 3 * width : 4 * width],
        dense[:, at + 2], dense[:, at + 3], dense[:, at + 4], dense[:, at + 5], dense[:, at + 6],
        dense[:, 4 * width : at],
        up_part, up_shift_part, down_part, down_shift_part,
    )


def solution(mesh):
    def step(*arrays):
        members, plane = mesh.shape["dp"], mesh.shape["expert"]
        fan = arrays[14].shape[0] // plane
        split = Mesh(mesh.devices.reshape(members // fan, fan, plane), ("hi", "lo", "expert"))
        every, dp = ("hi", "lo", "expert"), ("hi", "lo")
        in_specs = (
            (P(every, None),) * 4
            + (P(dp, None), P(dp), P(dp), P(dp, None), P(dp), P(dp), P(dp), P(dp), P(dp), P(dp, None))
            + (P("expert", None, None), P("expert", None), P("expert", None, None), P("expert", None))
        )
        out_specs = (
            (P(every, None),) * 3
            + (P(every), P(every), P(every, None))
            + (P(every),) * 5
            + (P(every, None), P("expert", dp, None), P("expert", dp), P("expert", dp, None), P("expert", dp))
        )

        return jax.shard_map(local, mesh=split, in_specs=in_specs, out_specs=out_specs, check_vma=False)(*arrays)

    return step
```
